512 devices in a mesh: gx: 16 (over y, x_hi), gy: 32 (over z, x_lo, core).
Axes of the slice: x: 4 (x_hi: 2, x_lo: 2; x = x_hi * 2 + x_lo), y: 8, z: 8, core: 2. Of those that a mesh axis runs over, the one named last changes fastest.
Arguments:
- right_side: float32 [262144, 64], P(('gx', 'gy')), may hold values from -6 to 6
- leaf_inverse: float32 [262144, 512], P(('gx', 'gy')), as said below
- basis_one: float32 [262144, 128], P(('gx', 'gy')), may hold values from -0.015625 to 0.015625
- basis_two: float32 [262144, 128], P(('gx', 'gy')), may hold values from -0.0234375 to 0.0234375
- factor_one: bfloat16 [1, 256, 256], replicated, may hold values from -0.5 to 0.5
- factor_two: bfloat16 [2, 256, 256], replicated, may hold values from -0.5 to 0.5
Outputs:
- solution: float32 [262144, 64], P(('gx', 'gy'))
The draws below stay inside these ranges and needn't reach their ends.
Inputs may be any that keep to these rules, and one draw needn't show every extreme that they name: `leaf_inverse`: each block of 512 consecutive rows is a symmetric positive definite 512 x 512 matrix.
All inputs are finite; a program needn't handle non-finite values.
Results may differ from the reference program's by a relative error of at most 0.0003.
Values sent between devices are 32-bit elements; how exact they have to be, the bound alone decides.
A program may use at most 64 MiB of HBM per device.

```python
import jax
import jax.numpy as jnp
from jax import lax

LEAF = 512
R = 128
NRHS = 64
LEVELS = 2
NROWS = 262144


def draw_leaf_inverse(key, part):
    block_count = NROWS // LEAF
    inner = LEAF // 4
    first, second = jax.random.split(jax.random.fold_in(key, 11))
    mixing = jax.random.normal(first, (block_count, LEAF, inner), jnp.float32)
    scales = jnp.exp(jax.random.uniform(second, (block_count, LEAF), jnp.float32, -0.3, 0.3))
    core = jnp.einsum('bik,bjk->bij', mixing, mixing) / inner + 0.5 * jnp.eye(LEAF, dtype=jnp.float32)
    scaled = scales[:, :, None] * core * scales[:, None, :]
    return scaled.reshape(NROWS, LEAF).astype(jnp.float32)


def block_scale(key, extent, pieces, least, high):
    factor_of = 1.0
    for axis_at, blocks in pieces:
        heights = jax.random.uniform(jax.random.fold_in(jax.random.fold_in(key, 6), axis_at), (blocks,), jnp.float32, least / len(pieces), high / len(pieces))
        factor_of = factor_of * jnp.repeat(jnp.exp(heights), extent[axis_at] // blocks).reshape((-1,) + (1,) * (len(extent) - 1 - axis_at))
    return factor_of


def centred(rng, dims, scale, bound, cuts=(), kind=jnp.bfloat16):
    result = scale * jax.random.normal(rng, dims, jnp.float32)
    if cuts:
        result = result * block_scale(rng, dims, cuts, -0.22, 0.18)
    return jnp.clip(result, -bound, bound).astype(kind)


def setup_inputs(seed: int = 0) -> dict:
    splits = jax.random.split(jax.random.key(seed), 7)
    return {
        "right_side": centred(splits[0], (NROWS, NRHS), 1.0, 6.0, ((0, 512),), jnp.float32),
        "leaf_inverse": draw_leaf_inverse(jax.random.fold_in(splits[6], 71), 0),
        "basis_one": centred(splits[2], (NROWS, R), (NROWS // 2) ** -0.5, 0.015625, ((0, 512),), jnp.float32),
        "basis_two": centred(splits[3], (NROWS, R), (NROWS // 4) ** -0.5, 0.0234375, ((0, 512),), jnp.float32),
        "factor_one": centred(splits[4], (1, 2 * R, 2 * R), R ** -0.5, 0.5),
        "factor_two": centred(splits[5], (2, 2 * R, 2 * R), R ** -0.5, 0.5),
    }


HIGH = lax.Precision.HIGHEST

def solve_small(matrix, right_terms):
    lower_factor = jnp.linalg.cholesky(matrix)
    middle = lax.linalg.triangular_solve(lower_factor, right_terms, left_side=True, lower=True)
    return lax.linalg.triangular_solve(lower_factor, middle, left_side=True, lower=True, transpose_a=True)

def reference(right_side, leaf_inverse, basis_one, basis_two, factor_one, factor_two):
    level_bases = (basis_one, basis_two)
    factors = (factor_one, factor_two)
    block_count = NROWS // LEAF
    stacked = jnp.concatenate((right_side,) + level_bases, axis=1).reshape(block_count, LEAF, -1)
    current = jnp.einsum('bij,bjc->bic', leaf_inverse.reshape(block_count, LEAF, LEAF), stacked, precision=HIGH)
    identity = jnp.eye(2 * R, dtype=jnp.float32)
    for level_index in range(LEVELS, 0, -1):
        width_used = NRHS + (level_index - 1) * R
        group_count = 2 ** level_index
        remaining = current[:, :, :width_used].reshape(group_count, -1, width_used)
        solved = current[:, :, width_used:width_used + R].reshape(group_count, -1, R)
        basis_rows = level_bases[level_index - 1].reshape(group_count, -1, R)
        gram_local = jnp.einsum('bnr,bns->brs', basis_rows, solved, precision=HIGH)
        projection = jnp.einsum('bnr,bnc->brc', basis_rows, remaining, precision=HIGH)
        factor = factors[level_index - 1].astype(jnp.float32).reshape(group_count // 2, 2, R, 2 * R)
        gram_pairs = gram_local.reshape(group_count // 2, 2, R, R)
        capacitance = identity + jnp.einsum('phra,phrs,phsb->pab', factor, gram_pairs, factor, precision=HIGH)
        right_terms = jnp.einsum('phra,phrc->pac', factor, projection.reshape(group_count // 2, 2, R, width_used), precision=HIGH)
        coefficient = solve_small(capacitance, right_terms)
        update = jnp.einsum('phra,pac->phrc', factor, coefficient, precision=HIGH).reshape(group_count, R, width_used)
        remaining = remaining - jnp.einsum('bnr,brc->bnc', solved, update, precision=HIGH)
        current = remaining.reshape(block_count, LEAF, width_used)
    return current.reshape(NROWS, NRHS)
```

```python
import functools

import jax
import jax.numpy as jnp
from jax import lax
from jax.experimental import pallas as pl
from jax.experimental.pallas import tpu as pltpu
from jax.sharding import PartitionSpec as P

MESH = pl.DeviceIdType.MESH
F32 = jnp.float32
BF16 = jnp.bfloat16
RANK = 128
NZ, NX, NY = 8, 4, 8


def split2(value):
    high = value.astype(BF16)
    return high, (value - high.astype(F32)).astype(BF16)


def dot(left, right, dims):
    return lax.dot_general(left, right, (dims, ((), ())), preferred_element_type=F32)


NN = ((1,), (0,))
TN = ((0,), (0,))


def mm(left, right, dims=NN):
    left_high, left_low = split2(left)
    right_high, right_low = split2(right)
    return dot(left_high, right_high, dims) + (
        dot(left_high, right_low, dims) + dot(left_low, right_high, dims)
    )


def mm_exact_left(left, right, dims=NN):
    right_high, right_low = split2(right)
    return dot(left, right_high, dims) + dot(left, right_low, dims)


def mm_exact_right(left, right, dims=NN):
    left_high, left_low = split2(left)
    return dot(left_high, right, dims) + dot(left_low, right, dims)


def local_kernel(rhs_ref, inv_ref, one_ref, two_ref, prod_ref, s1_ref, s2_ref, x_ref):
    one, two, rhs = one_ref[...], two_ref[...], rhs_ref[...]
    inv = inv_ref[...]
    s2 = mm(inv, two)
    s1 = mm(inv, one)
    x = mm(inv, rhs)
    s1_ref[...] = s1
    s2_ref[...] = s2
    x_ref[...] = x
    prod_ref[0] = mm(two, s2, TN)
    prod_ref[1] = mm(two, s1, TN)
    prod_ref[2] = mm(one, s1, TN)
    prod_ref[3, :, :64] = mm(two, x, TN)
    prod_ref[3, :, 64:] = mm(one, x, TN)


def comm_kernel(
    prod_ref, buf_ref,
    from_core, chip_sum, from_z, z_sum, from_x, x_sum, by_y,
    core_s, core_r, z_s, z_r, x_s, x_r, y_s, y_r,
    gx_s, gx_r, gz_s, gz_r, gc_s, gc_r,
):
    gx, gy = lax.axis_index("gx"), lax.axis_index("gy")
    y, x_hi = lax.div(gx, 2), lax.rem(gx, 2)
    z, x_lo, core = lax.div(gy, 4), lax.rem(lax.div(gy, 2), 2), lax.rem(gy, 2)
    x = x_hi * 2 + x_lo
    other = 1 - core
    sibling = (gx, gy + 1 - 2 * core)

    def z_peer(step):
        there = lax.rem(z + step, NZ)
        return there, (gx, there * 4 + x_lo * 2 + core)

    def x_peer(step):
        there = lax.rem(x + step, NX)
        return there, (y * 2 + lax.div(there, 2), z * 4 + lax.rem(there, 2) * 2 + core)

    def y_peer(step):
        there = lax.rem(y + step, NY)
        return there, (there * 2 + x_hi, gy)

    barrier = pltpu.get_barrier_semaphore()
    peers = [sibling]
    peers += [z_peer(step)[1] for step in range(1, NZ)]
    peers += [x_peer(step)[1] for step in range(1, NX)]
    peers += [y_peer(step)[1] for step in range(1, NY)]
    for peer in peers:
        pl.semaphore_signal(barrier, inc=1, device_id=peer, device_id_type=MESH)
    pl.semaphore_wait(barrier, len(peers))

    def send(source, target, send_sem, recv_sem, peer):
        copy = pltpu.make_async_remote_copy(
            src_ref=source, dst_ref=target, send_sem=send_sem, recv_sem=recv_sem,
            device_id=peer, device_id_type=MESH,
        )
        copy.start()
        return copy

    first = send(prod_ref.at[other], from_core, core_s, core_r, sibling)
    first.wait()
    chip_sum[...] = prod_ref[core] + from_core[...]

    copies = []
    for step in range(1, NZ):
        there, peer = z_peer(step)
        copies.append(send(chip_sum.at[there], from_z.at[step - 1], z_s.at[step - 1], z_r.at[step - 1], peer))
    total = chip_sum[z]
    for step, copy in enumerate(copies):
        copy.wait()
        total = total + from_z[step]
    z_sum[...] = total

    copies = []
    for step in range(1, NX):
        there, peer = x_peer(step)
        copies.append(send(z_sum.at[there], from_x.at[step - 1], x_s.at[step - 1], x_r.at[step - 1], peer))
    total = z_sum[x]
    for step, copy in enumerate(copies):
        copy.wait()
        total = total + from_x[step]
    x_sum[...] = total

    copies = []
    for step in range(1, NY):
        _, peer = y_peer(step)
        copies.append(send(x_sum, by_y.at[y], y_s.at[step - 1], y_r.at[step - 1], peer))
    by_y[y] = total
    for copy in copies:
        copy.wait()
    for slab in range(NY // 2):
        buf_ref[core, z, x, slab] = by_y[2 * slab] + by_y[2 * slab + 1]

    copies = []
    mine = buf_ref.at[core, z, x]
    for step in range(1, NX):
        _, peer = x_peer(step)
        copies.append(send(mine, mine, gx_s.at[step - 1], gx_r.at[step - 1], peer))
    for copy in copies:
        copy.wait()

    copies = []
    plane = buf_ref.at[core, z]
    for step in range(1, NZ):
        _, peer = z_peer(step)
        copies.append(send(plane, plane, gz_s.at[step - 1], gz_r.at[step - 1], peer))
    relays = [send(plane, plane, gc_s.at[0], gc_r.at[0], sibling)]
    for step, copy in enumerate(copies):
        copy.wait()
        origin = lax.rem(z + NZ - (step + 1), NZ)
        part = buf_ref.at[core, origin]
        relays.append(send(part, part, gc_s.at[step + 1], gc_r.at[step + 1], sibling))
    for relay in relays:
        relay.wait()


def sublane():
    return lax.broadcasted_iota(jnp.int32, (8, RANK), 0)


def lane():
    return lax.broadcasted_iota(jnp.int32, (8, RANK), 1)


def row_of(tile, index):
    return jnp.broadcast_to(tile[index : index + 1, :], tile.shape)


def reciprocal(value):
    guess = pl.reciprocal(value, approx=True)
    guess = guess * (2.0 - value * guess)
    return guess * (2.0 - value * guess)


def invert_in_place(work_ref, count):
    def panel_step(panel, carry):
        rows = lax.broadcasted_iota(jnp.int32, (8, RANK), 0)
        lanes = lax.broadcasted_iota(jnp.int32, (8, RANK), 1)
        base = panel * 8
        in_panel = jnp.logical_and(lanes >= base, lanes < base + 8)
        unit = (lanes - base == rows).astype(F32)
        picks = [jnp.full((8, RANK), base + j, jnp.int32) for j in range(8)]
        at = pl.ds(pl.multiple_of(base, 8), 8)
        for which in range(count):
            tile = work_ref[which, at, :]
            cols = [jnp.take_along_axis(tile, picks[j], axis=1) for j in range(8)]
            tile = jnp.where(in_panel, unit, tile)
            scale = jnp.ones((8, RANK), F32)
            for k in range(8):
                inverse = reciprocal(row_of(cols[k], k))
                scale = jnp.where(rows == k, inverse, scale)
                multiplier = jnp.where(rows == k, 0.0, cols[k]) * inverse
                for j in range(k + 1, 8):
                    cols[j] = cols[j] - multiplier * row_of(cols[j], k)
                tile = tile - multiplier * row_of(tile, k)
            tile = tile * scale
            tile_rows = [row_of(tile, j) for j in range(8)]
            for other in range(RANK // 8):
                here = work_ref[which, other * 8 : other * 8 + 8, :]
                update = jnp.where(in_panel, 0.0, here)
                for j in range(8):
                    update = update - jnp.take_along_axis(here, picks[j], axis=1) * tile_rows[j]
                work_ref[which, other * 8 : other * 8 + 8, :] = update
            work_ref[which, at, :] = tile
        return carry

    lax.fori_loop(0, RANK // 8, panel_step, 0)


def solve_kernel(buf_ref, one_ref, two_ref, s1_ref, s2_ref, x_ref, out_ref, work_ref, coef_ref):
    gx = lax.axis_index("gx")
    my_block = lax.div(gx, 4)
    my_pair, my_half = lax.div(my_block, 2), lax.rem(my_block, 2)

    def part(index, slab):
        whole = buf_ref[index // 2, (index % 2) * 4 : (index % 2) * 4 + 4, :, slab]
        return whole.reshape(RANK, RANK)

    def capacitance(factor, grams):
        top = mm_exact_right(grams[0], factor[:RANK])
        low = mm_exact_right(grams[1], factor[RANK:])
        cap = mm_exact_left(factor, jnp.concatenate((top, low), axis=0), TN)
        return cap

    eye = (
        lax.broadcasted_iota(jnp.int32, (RANK, RANK), 0)
        == lax.broadcasted_iota(jnp.int32, (RANK, RANK), 1)
    ).astype(F32)

    def solve(caps, terms, finish):
        count = len(caps)
        for q in range(count):
            work_ref[q] = caps[q][:RANK, :RANK] + eye
        invert_in_place(work_ref, count)
        firsts, crosses, wides, rests = [], [], [], []
        for q in range(count):
            inverse = work_ref[q]
            cross = caps[q][:RANK, RANK:]
            wide = mm(inverse, cross)
            first = mm(inverse, terms[q][:RANK])
            work_ref[q] = caps[q][RANK:, RANK:] + eye - mm(cross, wide, TN)
            rests.append(terms[q][RANK:] - mm(cross, first, TN))
            firsts.append(first)
            wides.append(wide)
        invert_in_place(work_ref, count)
        result = []
        for q in range(count):
            low = mm(work_ref[q], rests[q])
            top = firsts[q] - mm(wides[q], low)
            result.append((top, low))
        return result

    caps, terms = [], []
    for pair in range(2):
        factor = two_ref[pair]
        caps.append(capacitance(factor, [part(0, 2 * pair), part(0, 2 * pair + 1)]))
        sides = [
            jnp.concatenate((part(1, 2 * pair + half), part(3, 2 * pair + half)), axis=1)
            for half in range(2)
        ]
        terms.append(mm_exact_left(factor, jnp.concatenate(sides, axis=0), TN))
    result = solve(caps, terms, None)
    grams, projs = [], []
    for pair in range(2):
        top, low = result[pair]
        coef_ref[pair, :RANK] = top
        coef_ref[pair, RANK:] = low
        term = terms[pair]
        inner = mm(term[:RANK, :RANK], top, TN) + mm(term[RANK:, :RANK], low, TN)
        grams.append(part(2, 2 * pair) + part(2, 2 * pair + 1) - inner[:, :RANK])
        side = part(3, 2 * pair) + part(3, 2 * pair + 1)
        projs.append(side[:, 64:] - inner[:, RANK : RANK + 64])
    factor = one_ref[0]
    cap = capacitance(factor, grams)
    term = mm_exact_left(factor, jnp.concatenate(projs, axis=0), TN)
    ((top, low),) = solve([cap], [term], None)
    coef = jnp.concatenate((top, low), axis=0)
    half_rows = pl.ds(pl.multiple_of(my_pair * RANK, RANK), RANK)
    m1 = mm_exact_left(one_ref[0, half_rows, :], coef)
    own = coef_ref[my_pair]
    inner = own[:, RANK : RANK + 64] - mm(own[:, :RANK], m1)
    block_rows = pl.ds(pl.multiple_of(my_half * RANK, RANK), RANK)
    m2 = mm_exact_left(two_ref[my_pair, block_rows, :], inner)
    out_ref[...] = x_ref[...] - mm(s1_ref[...], m1) - mm(s2_ref[...], m2)


def vmem():
    return pl.BlockSpec(memory_space=pltpu.VMEM)


def body(right_side, leaf_inverse, basis_one, basis_two, factor_one, factor_two):
    rows = right_side.shape[0]
    shape = jax.ShapeDtypeStruct
    prod, s1, s2, x = pl.pallas_call(
        local_kernel,
        out_shape=(
            shape((4, RANK, RANK), F32), shape((rows, RANK), F32),
            shape((rows, RANK), F32), shape((rows, 64), F32),
        ),
        in_specs=[vmem()] * 4,
        out_specs=(vmem(),) * 4,
        compiler_params=pltpu.CompilerParams(vmem_limit_bytes=24 << 20),
    )(right_side, leaf_inverse, basis_one, basis_two)
    dma = pltpu.SemaphoreType.DMA
    buf = pl.pallas_call(
        comm_kernel,
        out_shape=shape((2, NZ, NX, 4, 8, RANK), F32),
        in_specs=[vmem()],
        out_specs=vmem(),
        scratch_shapes=[
            pltpu.VMEM((NZ, NX, 8, RANK), F32),
            pltpu.VMEM((NZ, NX, 8, RANK), F32),
            pltpu.VMEM((NZ - 1, NX, 8, RANK), F32),
            pltpu.VMEM((NX, 8, RANK), F32),
            pltpu.VMEM((NX - 1, 8, RANK), F32),
            pltpu.VMEM((8, RANK), F32),
            pltpu.VMEM((NY, 8, RANK), F32),
            dma, dma, dma((7,)), dma((7,)), dma((3,)), dma((3,)), dma((7,)), dma((7,)),
            dma((3,)), dma((3,)), dma((7,)), dma((7,)), dma((8,)), dma((8,)),
        ],
        compiler_params=pltpu.CompilerParams(
            collective_id=0, has_side_effects=True, vmem_limit_bytes=16 << 20
        ),
    )(prod.reshape(2, NZ, NX, 8, RANK))
    return pl.pallas_call(
        solve_kernel,
        out_shape=shape((rows, 64), F32),
        in_specs=[vmem()] * 6,
        out_specs=vmem(),
        scratch_shapes=[
            pltpu.VMEM((2, RANK, RANK), F32),
            pltpu.VMEM((2, 2 * RANK, 2 * RANK), F32),
        ],
        compiler_params=pltpu.CompilerParams(vmem_limit_bytes=32 << 20),
    )(buf, factor_one, factor_two, s1, s2, x)


def solution(mesh):
    split = P(("gx", "gy"), None)
    return jax.shard_map(
        body, mesh=mesh, in_specs=(split, split, split, split, P(), P()),
        out_specs=split, check_vma=False,
    )
```

```python
import functools

import jax
import jax.numpy as jnp
from jax import lax
from jax.experimental import pallas as pl
from jax.experimental.pallas import tpu as pltpu
from jax.sharding import PartitionSpec as P

MESH = pl.DeviceIdType.MESH
F32 = jnp.float32
BF16 = jnp.bfloat16
RANK = 128
NZ, NX, NY = 8, 4, 8


def split2(value):
    high = value.astype(BF16)
    return high, (value - high.astype(F32)).astype(BF16)


def dot(left, right, dims):
    return lax.dot_general(left, right, (dims, ((), ())), preferred_element_type=F32)


NN = ((1,), (0,))
TN = ((0,), (0,))


def mm(left, right, dims=NN):
    left_high, left_low = split2(left)
    right_high, right_low = split2(right)
    return dot(left_high, right_high, dims) + (
        dot(left_high, right_low, dims) + dot(left_low, right_high, dims)
    )


def mm_exact_left(left, right, dims=NN):
    right_high, right_low = split2(right)
    return dot(left, right_high, dims) + dot(left, right_low, dims)


def mm_exact_right(left, right, dims=NN):
    left_high, left_low = split2(left)
    return dot(left_high, right, dims) + dot(left_low, right, dims)


def local_kernel(rhs_ref, inv_ref, one_ref, two_ref, prod_ref, s1_ref, s2_ref, x_ref):
    one, two, rhs = one_ref[...], two_ref[...], rhs_ref[...]
    inv = inv_ref[...]
    s2 = mm(inv, two)
    s1 = mm(inv, one)
    x = mm(inv, rhs)
    s1_ref[...] = s1
    s2_ref[...] = s2
    x_ref[...] = x
    prod_ref[0] = mm(two, s2, TN)
    prod_ref[1] = mm(two, s1, TN)
    prod_ref[2] = mm(one, s1, TN)
    prod_ref[3, :, :64] = mm(two, x, TN)
    prod_ref[3, :, 64:] = mm(one, x, TN)


def comm_kernel(
    prod_ref, buf_ref,
    from_core, chip_sum, from_z, z_sum, from_x, x_sum, by_y,
    core_s, core_r, z_s, z_r, x_s, x_r, y_s, y_r,
    gx_s, gx_r, gz_s, gz_r, gc_s, gc_r,
):
    gx, gy = lax.axis_index("gx"), lax.axis_index("gy")
    y, x_hi = lax.div(gx, 2), lax.rem(gx, 2)
    z, x_lo, core = lax.div(gy, 4), lax.rem(lax.div(gy, 2), 2), lax.rem(gy, 2)
    x = x_hi * 2 + x_lo
    other = 1 - core
    sibling = (gx, gy + 1 - 2 * core)

    def z_peer(step):
        there = lax.rem(z + step, NZ)
        return there, (gx, there * 4 + x_lo * 2 + core)

    def x_peer(step):
        there = lax.rem(x + step, NX)
        return there, (y * 2 + lax.div(there, 2), z * 4 + lax.rem(there, 2) * 2 + core)

    def y_peer(step):
        there = lax.rem(y + step, NY)
        return there, (there * 2 + x_hi, gy)

    barrier = pltpu.get_barrier_semaphore()
    peers = [sibling]
    peers += [z_peer(step)[1] for step in range(1, NZ)]
    peers += [x_peer(step)[1] for step in range(1, NX)]
    peers += [y_peer(step)[1] for step in range(1, NY)]
    for peer in peers:
        pl.semaphore_signal(barrier, inc=1, device_id=peer, device_id_type=MESH)
    pl.semaphore_wait(barrier, len(peers))

    def send(source, target, send_sem, recv_sem, peer):
        copy = pltpu.make_async_remote_copy(
            src_ref=source, dst_ref=target, send_sem=send_sem, recv_sem=recv_sem,
            device_id=peer, device_id_type=MESH,
        )
        copy.start()
        return copy

    first = send(prod_ref.at[other], from_core, core_s, core_r, sibling)
    first.wait()
    chip_sum[...] = prod_ref[core] + from_core[...]

    copies = []
    for step in range(1, NZ):
        there, peer = z_peer(step)
        copies.append(send(chip_sum.at[there], from_z.at[step - 1], z_s.at[step - 1], z_r.at[step - 1], peer))
    total = chip_sum[z]
    for step, copy in enumerate(copies):
        copy.wait()
        total = total + from_z[step]
    z_sum[...] = total

    copies = []
    for step in range(1, NX):
        there, peer = x_peer(step)
        copies.append(send(z_sum.at[there], from_x.at[step - 1], x_s.at[step - 1], x_r.at[step - 1], peer))
    total = z_sum[x]
    for step, copy in enumerate(copies):
        copy.wait()
        total = total + from_x[step]
    x_sum[...] = total

    copies = []
    for step in range(1, NY):
        _, peer = y_peer(step)
        copies.append(send(x_sum, by_y.at[y], y_s.at[step - 1], y_r.at[step - 1], peer))
    by_y[y] = total
    for copy in copies:
        copy.wait()
    for slab in range(NY // 2):
        buf_ref[core, z, x, slab] = by_y[2 * slab] + by_y[2 * slab + 1]

    copies = []
    mine = buf_ref.at[core, z, x]
    for step in range(1, NX):
        _, peer = x_peer(step)
        copies.append(send(mine, mine, gx_s.at[step - 1], gx_r.at[step - 1], peer))
    for copy in copies:
        copy.wait()

    copies = []
    plane = buf_ref.at[core, z]
    for step in range(1, NZ):
        _, peer = z_peer(step)
        copies.append(send(plane, plane, gz_s.at[step - 1], gz_r.at[step - 1], peer))
    relays = [send(plane, plane, gc_s.at[0], gc_r.at[0], sibling)]
    for step, copy in enumerate(copies):
        copy.wait()
        origin = lax.rem(z + NZ - (step + 1), NZ)
        part = buf_ref.at[core, origin]
        relays.append(send(part, part, gc_s.at[step + 1], gc_r.at[step + 1], sibling))
    for relay in relays:
        relay.wait()


def sublane():
    return lax.broadcasted_iota(jnp.int32, (8, RANK), 0)


def lane():
    return lax.broadcasted_iota(jnp.int32, (8, RANK), 1)


def row_of(tile, index):
    return jnp.broadcast_to(tile[index : index + 1, :], tile.shape)


def reciprocal(value):
    guess = pl.reciprocal(value, approx=True)
    guess = guess * (2.0 - value * guess)
    return guess * (2.0 - value * guess)


def panel_solve(tiles, cols, unit_rows):
    scale = [jnp.ones((8, RANK), F32)] * 2
    cols = [list(pair) for pair in cols]
    for k in range(16):
        at, sub = k // 8, k % 8
        inverse = reciprocal(row_of(cols[k][at], sub))
        here = unit_rows == sub
        scale[at] = jnp.where(here, inverse, scale[at])
        factors = list(cols[k])
        factors[at] = jnp.where(here, 0.0, factors[at])
        factors = [factor * inverse for factor in factors]
        for j in range(k + 1, 16):
            across = row_of(cols[j][at], sub)
            cols[j] = [cols[j][t] - factors[t] * across for t in range(2)]
        across = row_of(tiles[at], sub)
        tiles = [tiles[t] - factors[t] * across for t in range(2)]
    return [tiles[t] * scale[t] for t in range(2)]


def invert_in_place(work_ref, high_ref, low_ref, count):
    rows = lax.broadcasted_iota(jnp.int32, (8, RANK), 0)
    lanes = lax.broadcasted_iota(jnp.int32, (8, RANK), 1)
    tile_count = RANK // 8

    def apply_last(which, base_before, before):
        last = jnp.logical_and(lanes >= base_before, lanes < base_before + 16)
        whole = work_ref[which]
        left_high, left_low = split2(whole)
        high, low = high_ref[which], low_ref[which]
        update = dot(left_high, high, NN) + (dot(left_high, low, NN) + dot(left_low, high, NN))
        for tile in range(tile_count):
            at = slice(tile * 8, tile * 8 + 8)
            work_ref[which, at, :] = jnp.where(last, 0.0, whole[at]) - update[at]
        at = pl.ds(pl.multiple_of(jnp.maximum(base_before, 0), 16), 16)
        work_ref[which, at, :] = jnp.concatenate(before, axis=0)

    def step(panel, carry):
        base = panel * 16
        inside = jnp.logical_and(lanes >= base, lanes < base + 16)
        picks = [jnp.full((8, RANK), base + j, jnp.int32) for j in range(16)]
        following = jnp.minimum(base + 16, RANK - 16)
        after = []
        for which in range(count):
            current, before = carry[which]
            cols = [
                [jnp.take_along_axis(current[t], picks[j], axis=1) for t in range(2)]
                for j in range(16)
            ]
            tiles = [
                jnp.where(inside, (lanes - base == rows + 8 * t).astype(F32), current[t])
                for t in range(2)
            ]
            apply_last(which, base - 16, before)
            solved = panel_solve(tiles, cols, rows)
            joined = jnp.concatenate(solved, axis=0)
            high, low = split2(joined)
            gone = pl.ds(pl.multiple_of(jnp.maximum(base - 16, 0), 16), 16)
            high_ref[which, gone, :] = jnp.zeros((16, RANK), BF16)
            low_ref[which, gone, :] = jnp.zeros((16, RANK), BF16)
            at = pl.ds(pl.multiple_of(base, 16), 16)
            high_ref[which, at, :] = high
            low_ref[which, at, :] = low
            upcoming = []
            for t in range(2):
                tile = work_ref[which, pl.ds(pl.multiple_of(following + 8 * t, 8), 8), :]
                fresh = jnp.where(inside, 0.0, tile)
                for j in range(16):
                    weight = jnp.take_along_axis(tile, picks[j], axis=1)
                    fresh = fresh - weight * row_of(solved[j // 8], j % 8)
                upcoming.append(fresh)
            after.append((tuple(upcoming), tuple(solved)))
        return tuple(after)

    start = []
    for which in range(count):
        high_ref[which] = jnp.zeros((RANK, RANK), BF16)
        low_ref[which] = jnp.zeros((RANK, RANK), BF16)
        first = (work_ref[which, :8, :], work_ref[which, 8:16, :])
        start.append((first, first))
    done = lax.fori_loop(0, RANK // 16, step, tuple(start))
    for which in range(count):
        apply_last(which, RANK - 16, done[which][1])


def solve_kernel(buf_ref, one_ref, two_ref, s1_ref, s2_ref, x_ref, out_ref, work_ref, coef_ref, high_ref, low_ref):
    gx = lax.axis_index("gx")
    my_block = lax.div(gx, 4)
    my_pair, my_half = lax.div(my_block, 2), lax.rem(my_block, 2)

    def part(index, slab):
        whole = buf_ref[index // 2, (index % 2) * 4 : (index % 2) * 4 + 4, :, slab]
        return whole.reshape(RANK, RANK)

    def capacitance(factor, grams):
        top = mm_exact_right(grams[0], factor[:RANK])
        low = mm_exact_right(grams[1], factor[RANK:])
        cap = mm_exact_left(factor, jnp.concatenate((top, low), axis=0), TN)
        return cap

    eye = (
        lax.broadcasted_iota(jnp.int32, (RANK, RANK), 0)
        == lax.broadcasted_iota(jnp.int32, (RANK, RANK), 1)
    ).astype(F32)

    def solve(caps, terms, finish):
        count = len(caps)
        for q in range(count):
            work_ref[q] = caps[q][:RANK, :RANK] + eye
        invert_in_place(work_ref, high_ref, low_ref, count)
        firsts, crosses, wides, rests = [], [], [], []
        for q in range(count):
            inverse = work_ref[q]
            cross = caps[q][:RANK, RANK:]
            wide = mm(inverse, cross)
            first = mm(inverse, terms[q][:RANK])
            work_ref[q] = caps[q][RANK:, RANK:] + eye - mm(cross, wide, TN)
            rests.append(terms[q][RANK:] - mm(cross, first, TN))
            firsts.append(first)
            wides.append(wide)
        invert_in_place(work_ref, high_ref, low_ref, count)
        result = []
        for q in range(count):
            low = mm(work_ref[q], rests[q])
            top = firsts[q] - mm(wides[q], low)
            result.append((top, low))
        return result

    caps, terms = [], []
    for pair in range(2):
        factor = two_ref[pair]
        caps.append(capacitance(factor, [part(0, 2 * pair), part(0, 2 * pair + 1)]))
        sides = [
            jnp.concatenate((part(1, 2 * pair + half), part(3, 2 * pair + half)), axis=1)
            for half in range(2)
        ]
        terms.append(mm_exact_left(factor, jnp.concatenate(sides, axis=0), TN))
    result = solve(caps, terms, None)
    grams, projs = [], []
    for pair in range(2):
        top, low = result[pair]
        coef_ref[pair, :RANK] = top
        coef_ref[pair, RANK:] = low
        term = terms[pair]
        inner = mm(term[:RANK, :RANK], top, TN) + mm(term[RANK:, :RANK], low, TN)
        grams.append(part(2, 2 * pair) + part(2, 2 * pair + 1) - inner[:, :RANK])
        side = part(3, 2 * pair) + part(3, 2 * pair + 1)
        projs.append(side[:, 64:] - inner[:, RANK : RANK + 64])
    factor = one_ref[0]
    cap = capacitance(factor, grams)
    term = mm_exact_left(factor, jnp.concatenate(projs, axis=0), TN)
    ((top, low),) = solve([cap], [term], None)
    coef = jnp.concatenate((top, low), axis=0)
    half_rows = pl.ds(pl.multiple_of(my_pair * RANK, RANK), RANK)
    m1 = mm_exact_left(one_ref[0, half_rows, :], coef)
    own = coef_ref[my_pair]
    inner = own[:, RANK : RANK + 64] - mm(own[:, :RANK], m1)
    block_rows = pl.ds(pl.multiple_of(my_half * RANK, RANK), RANK)
    m2 = mm_exact_left(two_ref[my_pair, block_rows, :], inner)
    out_ref[...] = x_ref[...] - mm(s1_ref[...], m1) - mm(s2_ref[...], m2)


def vmem():
    return pl.BlockSpec(memory_space=pltpu.VMEM)


def body(right_side, leaf_inverse, basis_one, basis_two, factor_one, factor_two):
    rows = right_side.shape[0]
    shape = jax.ShapeDtypeStruct
    prod, s1, s2, x = pl.pallas_call(
        local_kernel,
        out_shape=(
            shape((4, RANK, RANK), F32), shape((rows, RANK), F32),
            shape((rows, RANK), F32), shape((rows, 64), F32),
        ),
        in_specs=[vmem()] * 4,
        out_specs=(vmem(),) * 4,
        compiler_params=pltpu.CompilerParams(vmem_limit_bytes=24 << 20),
    )(right_side, leaf_inverse, basis_one, basis_two)
    dma = pltpu.SemaphoreType.DMA
    buf = pl.pallas_call(
        comm_kernel,
        out_shape=shape((2, NZ, NX, 4, 8, RANK), F32),
        in_specs=[vmem()],
        out_specs=vmem(),
        scratch_shapes=[
            pltpu.VMEM((NZ, NX, 8, RANK), F32),
            pltpu.VMEM((NZ, NX, 8, RANK), F32),
            pltpu.VMEM((NZ - 1, NX, 8, RANK), F32),
            pltpu.VMEM((NX, 8, RANK), F32),
            pltpu.VMEM((NX - 1, 8, RANK), F32),
            pltpu.VMEM((8, RANK), F32),
            pltpu.VMEM((NY, 8, RANK), F32),
            dma, dma, dma((7,)), dma((7,)), dma((3,)), dma((3,)), dma((7,)), dma((7,)),
            dma((3,)), dma((3,)), dma((7,)), dma((7,)), dma((8,)), dma((8,)),
        ],
        compiler_params=pltpu.CompilerParams(
            collective_id=0, has_side_effects=True, vmem_limit_bytes=16 << 20
        ),
    )(prod.reshape(2, NZ, NX, 8, RANK))
    return run_solve(buf, factor_one, factor_two, s1, s2, x)


def run_solve(buf, factor_one, factor_two, s1, s2, x):
    return pl.pallas_call(
        solve_kernel,
        out_shape=jax.ShapeDtypeStruct(x.shape, F32),
        in_specs=[vmem()] * 6,
        out_specs=vmem(),
        scratch_shapes=[
            pltpu.VMEM((2, RANK, RANK), F32),
            pltpu.VMEM((2, 2 * RANK, 2 * RANK), F32),
            pltpu.VMEM((2, RANK, RANK), BF16),
            pltpu.VMEM((2, RANK, RANK), BF16),
        ],
        compiler_params=pltpu.CompilerParams(vmem_limit_bytes=32 << 20),
    )(buf, factor_one, factor_two, s1, s2, x)


def solution(mesh):
    split = P(("gx", "gy"), None)
    return jax.shard_map(
        body, mesh=mesh, in_specs=(split, split, split, split, P(), P()),
        out_specs=split, check_vma=False,
    )
```

```python
import functools

import jax
import jax.numpy as jnp
from jax import lax
from jax.experimental import pallas as pl
from jax.experimental.pallas import tpu as pltpu
from jax.sharding import PartitionSpec as P

MESH = pl.DeviceIdType.MESH
F32 = jnp.float32
BF16 = jnp.bfloat16
RANK = 128
NZ, NX, NY = 8, 4, 8


def split2(value):
    high = value.astype(BF16)
    return high, (value - high.astype(F32)).astype(BF16)


def dot(left, right, dims):
    return lax.dot_general(left, right, (dims, ((), ())), preferred_element_type=F32)


NN = ((1,), (0,))
TN = ((0,), (0,))
NT = ((1,), (1,))


def mm(left, right, dims=NN):
    left_high, left_low = split2(left)
    right_high, right_low = split2(right)
    return dot(left_high, right_high, dims) + (
        dot(left_high, right_low, dims) + dot(left_low, right_high, dims)
    )


def mm_exact_left(left, right, dims=NN):
    right_high, right_low = split2(right)
    return dot(left, right_high, dims) + dot(left, right_low, dims)


def mm_exact_right(left, right, dims=NN):
    left_high, left_low = split2(left)
    return dot(left_high, right, dims) + dot(left_low, right, dims)


def farthest_first(count):
    return sorted(range(1, count), key=lambda step: -min(step, count - step))


def local_products(inv, two, one, rhs_t, prod_ref, s_high_ref, s_low_ref, x_ref):
    both = jnp.concatenate((two, one), axis=1)
    both_high, both_low = split2(both)
    inv_high, inv_low = split2(inv)
    solved = dot(inv_high, both_high, NN) + (
        dot(inv_high, both_low, NN) + dot(inv_low, both_high, NN)
    )
    rhs_high, rhs_low = split2(rhs_t)
    x_t = dot(rhs_high, inv_high, NN) + (
        dot(rhs_high, inv_low, NN) + dot(rhs_low, inv_high, NN)
    )
    s_high, s_low = split2(solved)
    grams = dot(both_high, s_high, TN) + (dot(both_high, s_low, TN) + dot(both_low, s_high, TN))
    x_high, x_low = split2(x_t)
    projs = dot(x_high, both_high, NN) + (dot(x_high, both_low, NN) + dot(x_low, both_high, NN))
    shape = (2, NZ, 8, RANK)
    prod_ref[0, 0:2] = grams[:RANK, :RANK].reshape(shape)
    prod_ref[0, 2:4] = grams[:RANK, RANK:].reshape(shape)
    prod_ref[1, 0:2] = grams[RANK:, RANK:].reshape(shape)
    prod_ref[1, 2] = projs[:, :RANK].reshape(shape[1:])
    prod_ref[1, 3] = projs[:, RANK:].reshape(shape[1:])
    s_high_ref[...] = s_high
    s_low_ref[...] = s_low
    x_ref[...] = x_t


def gather_kernel(
    rhs_hbm, inv_hbm, one_hbm, two_hbm, buf_ref, s_high_ref, s_low_ref, x_ref,
    rhs_ref, inv_ref, one_ref, two_ref,
    prod_ref, from_core, chip_sum, from_z, z_sum, from_x, x_sum, by_y, away,
    in_s, core_s, core_r, z_s, z_r, x_s, x_r, y_s, y_r, w_s, w_r, gz_s, gz_r, gx_s, gx_r,
):
    gx, gy = lax.axis_index("gx"), lax.axis_index("gy")
    y, x_hi = lax.div(gx, 2), lax.rem(gx, 2)
    z, x_lo, core = lax.div(gy, 4), lax.rem(lax.div(gy, 2), 2), lax.rem(gy, 2)
    x = x_hi * 2 + x_lo
    other = 1 - core
    sibling = (gx, gy + 1 - 2 * core)

    def z_peer(step):
        there = lax.rem(z + step, NZ)
        return there, (gx, there * 4 + x_lo * 2 + core)

    def x_peer(step):
        there = lax.rem(x + step, NX)
        return there, (y * 2 + lax.div(there, 2), z * 4 + lax.rem(there, 2) * 2 + core)

    def y_peer(step):
        there = lax.rem(y + step, NY)
        return there, (there * 2 + x_hi, gy)

    barrier = pltpu.get_barrier_semaphore()
    peers = [z_peer(step)[1] for step in farthest_first(NZ)]
    peers += [y_peer(step)[1] for step in farthest_first(NY)]
    peers += [x_peer(step)[1] for step in farthest_first(NX)]
    peers += [sibling]
    for peer in peers:
        pl.semaphore_signal(barrier, inc=1, device_id=peer, device_id_type=MESH)

    loads = [
        pltpu.make_async_copy(source, target, in_s.at[index])
        for index, (source, target) in enumerate(
            ((inv_hbm, inv_ref), (two_hbm, two_ref), (one_hbm, one_ref), (rhs_hbm, rhs_ref))
        )
    ]
    for load in loads:
        load.start()
    for load in loads:
        load.wait()
    local_products(
        inv_ref[...], two_ref[...], one_ref[...], rhs_ref[...],
        prod_ref, s_high_ref, s_low_ref, x_ref,
    )
    pl.semaphore_wait(barrier, len(peers))

    def send(source, target, send_sem, recv_sem, peer):
        copy = pltpu.make_async_remote_copy(
            src_ref=source, dst_ref=target, send_sem=send_sem, recv_sem=recv_sem,
            device_id=peer, device_id_type=MESH,
        )
        copy.start()
        return copy

    first = send(prod_ref.at[other], from_core, core_s, core_r, sibling)
    first.wait()
    for there in range(NX):
        chip_sum[:, there] = prod_ref[core, there] + from_core[there]

    copies = []
    for step in farthest_first(NZ):
        there, peer = z_peer(step)
        at = step - 1
        copies.append(send(chip_sum.at[there], from_z.at[at], z_s.at[at], z_r.at[at], peer))
    total = chip_sum[z]
    for copy in copies:
        copy.wait()
    for step in range(NZ - 1):
        total = total + from_z[step]
    z_sum[...] = total

    copies = []
    for step in farthest_first(NX):
        there, peer = x_peer(step)
        at = step - 1
        copies.append(send(z_sum.at[there], from_x.at[at], x_s.at[at], x_r.at[at], peer))
    total = z_sum[x]
    for copy in copies:
        copy.wait()
    for step in range(NX - 1):
        total = total + from_x[step]
    x_sum[...] = total

    copies = []
    for step in farthest_first(NY):
        _, peer = y_peer(step)
        copies.append(send(x_sum, by_y.at[y], y_s.at[step - 1], y_r.at[step - 1], peer))
    by_y[y] = total
    for copy in copies:
        copy.wait()
    for slab in range(2):
        here, there = core * 4 + 2 * slab, other * 4 + 2 * slab
        away[slab] = by_y[there] + by_y[there + 1]
        buf_ref[x, z, core, slab] = by_y[here] + by_y[here + 1]
    send(away, buf_ref.at[x, z, core], w_s, w_r, sibling).wait()

    for place, step_peer, count, sends, receives in (
        (buf_ref.at[x, z], z_peer, NZ, gz_s, gz_r),
        (buf_ref.at[x], x_peer, NX, gx_s, gx_r),
    ):
        copies = []
        for step in farthest_first(count):
            _, peer = step_peer(step)
            copies.append(send(place, place, sends.at[step - 1], receives.at[step - 1], peer))
        for copy in copies:
            copy.wait()


def row_of(tile, index):
    return jnp.broadcast_to(tile[index : index + 1, :], tile.shape)


def reciprocal(value):
    guess = pl.reciprocal(value, approx=True)
    guess = guess * (2.0 - value * guess)
    return guess * (2.0 - value * guess)


def panel_solve(tiles, cols, unit_rows):
    scale = [jnp.ones((8, RANK), F32)] * 2
    cols = [list(pair) for pair in cols]
    for k in range(16):
        at, sub = k // 8, k % 8
        inverse = reciprocal(row_of(cols[k][at], sub))
        here = unit_rows == sub
        scale[at] = jnp.where(here, inverse, scale[at])
        factors = list(cols[k])
        factors[at] = jnp.where(here, 0.0, factors[at])
        factors = [factor * inverse for factor in factors]
        for j in range(k + 1, 16):
            across = row_of(cols[j][at], sub)
            cols[j] = [cols[j][t] - factors[t] * across for t in range(2)]
        across = row_of(tiles[at], sub)
        tiles = [tiles[t] - factors[t] * across for t in range(2)]
    return [tiles[t] * scale[t] for t in range(2)]


def invert_in_place(work_ref, high_ref, low_ref, count):
    rows = lax.broadcasted_iota(jnp.int32, (8, RANK), 0)
    lanes = lax.broadcasted_iota(jnp.int32, (8, RANK), 1)
    tile_count = RANK // 8

    def apply_last(which, base_before, before):
        last = jnp.logical_and(lanes >= base_before, lanes < base_before + 16)
        whole = work_ref[which]
        left_high, left_low = split2(whole)
        high, low = high_ref[which], low_ref[which]
        update = dot(left_high, high, NN) + (dot(left_high, low, NN) + dot(left_low, high, NN))
        for tile in range(tile_count):
            at = slice(tile * 8, tile * 8 + 8)
            work_ref[which, at, :] = jnp.where(last, 0.0, whole[at]) - update[at]
        at = pl.ds(pl.multiple_of(jnp.maximum(base_before, 0), 16), 16)
        work_ref[which, at, :] = jnp.concatenate(before, axis=0)

    def step(panel, carry):
        base = panel * 16
        inside = jnp.logical_and(lanes >= base, lanes < base + 16)
        picks = [jnp.full((8, RANK), base + j, jnp.int32) for j in range(16)]
        following = jnp.minimum(base + 16, RANK - 16)
        after = []
        for which in range(count):
            current, before = carry[which]
            cols = [
                [jnp.take_along_axis(current[t], picks[j], axis=1) for t in range(2)]
                for j in range(16)
            ]
            tiles = [
                jnp.where(inside, (lanes - base == rows + 8 * t).astype(F32), current[t])
                for t in range(2)
            ]
            apply_last(which, base - 16, before)
            solved = panel_solve(tiles, cols, rows)
            joined = jnp.concatenate(solved, axis=0)
            high, low = split2(joined)
            gone = pl.ds(pl.multiple_of(jnp.maximum(base - 16, 0), 16), 16)
            high_ref[which, gone, :] = jnp.zeros((16, RANK), BF16)
            low_ref[which, gone, :] = jnp.zeros((16, RANK), BF16)
            at = pl.ds(pl.multiple_of(base, 16), 16)
            high_ref[which, at, :] = high
            low_ref[which, at, :] = low
            upcoming = []
            for t in range(2):
                tile = work_ref[which, pl.ds(pl.multiple_of(following + 8 * t, 8), 8), :]
                fresh = jnp.where(inside, 0.0, tile)
                for j in range(16):
                    weight = jnp.take_along_axis(tile, picks[j], axis=1)
                    fresh = fresh - weight * row_of(solved[j // 8], j % 8)
                upcoming.append(fresh)
            after.append((tuple(upcoming), tuple(solved)))
        return tuple(after)

    start = []
    for which in range(count):
        high_ref[which] = jnp.zeros((RANK, RANK), BF16)
        low_ref[which] = jnp.zeros((RANK, RANK), BF16)
        first = (work_ref[which, :8, :], work_ref[which, 8:16, :])
        start.append((first, first))
    done = lax.fori_loop(0, RANK // 16, step, tuple(start))
    for which in range(count):
        apply_last(which, RANK - 16, done[which][1])


def part(buf_ref, index, slab):
    start = (index % 2) * 2
    return buf_ref[start : start + 2, :, index // 2, slab].reshape(RANK, RANK)


def capacitance(factor, grams):
    top = mm_exact_right(grams[0], factor[:RANK])
    low = mm_exact_right(grams[1], factor[RANK:])
    return mm_exact_left(factor, jnp.concatenate((top, low), axis=0), TN)


def solve(cap, term, work_ref, high_ref, low_ref):
    eye = (
        lax.broadcasted_iota(jnp.int32, (RANK, RANK), 0)
        == lax.broadcasted_iota(jnp.int32, (RANK, RANK), 1)
    ).astype(F32)
    work_ref[0] = cap[:RANK, :RANK] + eye
    invert_in_place(work_ref, high_ref, low_ref, 1)
    inverse = work_ref[0]
    cross = cap[:RANK, RANK:]
    wide = mm(inverse, cross)
    work_ref[0] = cap[RANK:, RANK:] + eye - mm(cross, wide, TN)
    first = mm(inverse, term[:RANK])
    rest = term[RANK:] - mm(cross, first, TN)
    invert_in_place(work_ref, high_ref, low_ref, 1)
    low = mm(work_ref[0], rest)
    top = first - mm(wide, low)
    return top, low


def fine_kernel(buf_ref, two_ref, schur_ref, coef_ref, work_ref, high_ref, low_ref):
    pair = lax.rem(lax.axis_index("gy"), 2)
    factor = two_ref[pair]
    cap = capacitance(factor, [part(buf_ref, 0, 0), part(buf_ref, 0, 1)])
    rights = [part(buf_ref, 3, slab) for slab in range(2)]
    sides = [
        jnp.concatenate((part(buf_ref, 1, slab), rights[slab][:64].T), axis=1)
        for slab in range(2)
    ]
    term = mm_exact_left(factor, jnp.concatenate(sides, axis=0), TN)
    top, low = solve(cap, term, work_ref, high_ref, low_ref)
    coef_ref[:RANK] = top
    coef_ref[RANK:] = low
    inner = mm(term[:RANK, :RANK], top, TN) + mm(term[RANK:, :RANK], low, TN)
    schur_ref[:, :RANK] = part(buf_ref, 2, 0) + part(buf_ref, 2, 1) - inner[:, :RANK]
    schur_ref[:, RANK:] = (rights[0][64:] + rights[1][64:]).T - inner[:, RANK:]


def swap_kernel(schur_ref, coef_ref, schur_out, coef_out, sends, receives):
    gx, gy = lax.axis_index("gx"), lax.axis_index("gy")
    sibling = (gx, gy + 1 - 2 * lax.rem(gy, 2))
    barrier = pltpu.get_barrier_semaphore()
    pl.semaphore_signal(barrier, inc=1, device_id=sibling, device_id_type=MESH)
    pl.semaphore_wait(barrier, 1)
    copies = []
    for index, (source, target) in enumerate(((schur_ref, schur_out), (coef_ref, coef_out))):
        copy = pltpu.make_async_remote_copy(
            src_ref=source, dst_ref=target, send_sem=sends.at[index],
            recv_sem=receives.at[index], device_id=sibling, device_id_type=MESH,
        )
        copy.start()
        copies.append(copy)
    for copy in copies:
        copy.wait()


def coarse_kernel(
    schur_ref, coef_ref, schur_other, coef_other, one_ref, two_ref, s_high_ref, s_low_ref, x_ref,
    out_ref, schurs, coefs, work_ref, high_ref, low_ref,
):
    block = lax.div(lax.axis_index("gx"), 4)
    my_pair, my_half = lax.div(block, 2), lax.rem(block, 2)
    core = lax.rem(lax.axis_index("gy"), 2)
    schurs[core] = schur_ref[...]
    schurs[1 - core] = schur_other[...]
    coefs[core] = coef_ref[...]
    coefs[1 - core] = coef_other[...]
    factor = one_ref[0]
    cap = capacitance(factor, [schurs[0, :, :RANK], schurs[1, :, :RANK]])
    term = mm_exact_left(
        factor, jnp.concatenate((schurs[0, :, RANK:], schurs[1, :, RANK:]), axis=0), TN
    )
    top, low = solve(cap, term, work_ref, high_ref, low_ref)
    half_rows = pl.ds(pl.multiple_of(my_pair * RANK, RANK), RANK)
    m1 = mm_exact_left(one_ref[0, half_rows, :], jnp.concatenate((top, low), axis=0))
    own = coefs[my_pair]
    inner = own[:, RANK:] - mm(own[:, :RANK], m1)
    block_rows = pl.ds(pl.multiple_of(my_half * RANK, RANK), RANK)
    m2 = mm_exact_left(two_ref[my_pair, block_rows, :], inner)
    weights = jnp.concatenate((m2, m1), axis=0).T
    w_high, w_low = split2(weights)
    s_high = s_high_ref[...]
    out_ref[...] = x_ref[...] - (
        dot(w_high, s_high, NT) + (dot(w_high, s_low_ref[...], NT) + dot(w_low, s_high, NT))
    )


def vmem():
    return pl.BlockSpec(memory_space=pltpu.VMEM)


def shape(*dims, kind=F32):
    return jax.ShapeDtypeStruct(dims, kind)


def inverse_scratch():
    return [
        pltpu.VMEM((1, RANK, RANK), F32),
        pltpu.VMEM((1, RANK, RANK), BF16),
        pltpu.VMEM((1, RANK, RANK), BF16),
    ]


def run_gather(rhs_t, leaf_inverse, basis_one, basis_two):
    rows = leaf_inverse.shape[0]
    dma = pltpu.SemaphoreType.DMA
    return pl.pallas_call(
        gather_kernel,
        out_shape=(
            shape(NX, NZ, 2, 2, 8, RANK), shape(rows, 2 * RANK, kind=BF16),
            shape(rows, 2 * RANK, kind=BF16), shape(64, rows),
        ),
        in_specs=[pl.BlockSpec(memory_space=pltpu.HBM)] * 4,
        out_specs=(vmem(),) * 4,
        scratch_shapes=[
            pltpu.VMEM((64, rows), F32),
            pltpu.VMEM((rows, rows), F32),
            pltpu.VMEM((rows, RANK), F32),
            pltpu.VMEM((rows, RANK), F32),
            pltpu.VMEM((2, NX, NZ, 8, RANK), F32),
            pltpu.VMEM((NX, NZ, 8, RANK), F32),
            pltpu.VMEM((NZ, NX, 8, RANK), F32),
            pltpu.VMEM((NZ - 1, NX, 8, RANK), F32),
            pltpu.VMEM((NX, 8, RANK), F32),
            pltpu.VMEM((NX - 1, 8, RANK), F32),
            pltpu.VMEM((8, RANK), F32),
            pltpu.VMEM((NY, 8, RANK), F32),
            pltpu.VMEM((2, 8, RANK), F32),
            dma((4,)), dma, dma, dma((7,)), dma((7,)), dma((3,)), dma((3,)), dma((7,)), dma((7,)),
            dma, dma, dma((7,)), dma((7,)), dma((3,)), dma((3,)),
        ],
        compiler_params=pltpu.CompilerParams(
            collective_id=0, has_side_effects=True, vmem_limit_bytes=62 << 20
        ),
    )(rhs_t, leaf_inverse, basis_one, basis_two)


def run_fine(buf, factor_two):
    return pl.pallas_call(
        fine_kernel,
        out_shape=(shape(RANK, 192), shape(2 * RANK, 192)),
        in_specs=[vmem()] * 2,
        out_specs=(vmem(),) * 2,
        scratch_shapes=inverse_scratch(),
        compiler_params=pltpu.CompilerParams(vmem_limit_bytes=32 << 20),
    )(buf, factor_two)


def run_swap(schur, coef):
    dma = pltpu.SemaphoreType.DMA
    return pl.pallas_call(
        swap_kernel,
        out_shape=(shape(*schur.shape), shape(*coef.shape)),
        in_specs=[vmem()] * 2,
        out_specs=(vmem(),) * 2,
        scratch_shapes=[dma((2,)), dma((2,))],
        compiler_params=pltpu.CompilerParams(
            collective_id=1, has_side_effects=True, vmem_limit_bytes=16 << 20
        ),
    )(schur, coef)


def run_coarse(schur, coef, schur_other, coef_other, factor_one, factor_two, s_high, s_low, x_t):
    return pl.pallas_call(
        coarse_kernel,
        out_shape=shape(*x_t.shape),
        in_specs=[vmem()] * 9,
        out_specs=vmem(),
        scratch_shapes=[
            pltpu.VMEM((2, RANK, 192), F32),
            pltpu.VMEM((2, 2 * RANK, 192), F32),
        ] + inverse_scratch(),
        compiler_params=pltpu.CompilerParams(vmem_limit_bytes=32 << 20),
    )(schur, coef, schur_other, coef_other, factor_one, factor_two, s_high, s_low, x_t)


def body(right_side, leaf_inverse, basis_one, basis_two, factor_one, factor_two):
    buf, s_high, s_low, x_t = run_gather(right_side.T, leaf_inverse, basis_one, basis_two)
    schur, coef = run_fine(buf, factor_two)
    schur_other, coef_other = run_swap(schur, coef)
    out_t = run_coarse(
        schur, coef, schur_other, coef_other, factor_one, factor_two, s_high, s_low, x_t
    )
    return out_t.T


def solution(mesh):
    split = P(("gx", "gy"), None)
    return jax.shard_map(
        body, mesh=mesh, in_specs=(split, split, split, split, P(), P()),
        out_specs=split, check_vma=False,
    )
```

```python
import functools

import jax
import jax.numpy as jnp
from jax import lax
from jax.experimental import pallas as pl
from jax.experimental.pallas import tpu as pltpu
from jax.sharding import PartitionSpec as P

MESH = pl.DeviceIdType.MESH
F32 = jnp.float32
BF16 = jnp.bfloat16
RANK = 128
NZ, NX, NY = 8, 4, 8


def split2(value):
    high = value.astype(BF16)
    return high, (value - high.astype(F32)).astype(BF16)


def dot(left, right, dims):
    return lax.dot_general(left, right, (dims, ((), ())), preferred_element_type=F32)


NN = ((1,), (0,))
TN = ((0,), (0,))
NT = ((1,), (1,))


def mm(left, right, dims=NN):
    left_high, left_low = split2(left)
    right_high, right_low = split2(right)
    return dot(left_high, right_high, dims) + (
        dot(left_high, right_low, dims) + dot(left_low, right_high, dims)
    )


def mm_exact_left(left, right, dims=NN):
    right_high, right_low = split2(right)
    return dot(left, right_high, dims) + dot(left, right_low, dims)


def mm_exact_right(left, right, dims=NN):
    left_high, left_low = split2(left)
    return dot(left_high, right, dims) + dot(left_low, right, dims)


def away(step, count):
    return min(step, count - step)


def farthest_first(count):
    return sorted(range(1, count), key=lambda step: -away(step, count))


def plane_steps():
    steps = [(up, over) for up in range(NZ) for over in range(NX) if up or over]
    return sorted(steps, key=lambda step: -away(step[0], NZ) - away(step[1], NX))


def local_products(inv, two, one, rhs_t, prod_ref, s_high_ref, s_low_ref, x_ref):
    both = jnp.concatenate((two, one), axis=1)
    both_high, both_low = split2(both)
    inv_high, inv_low = split2(inv)
    solved = dot(inv_high, both_high, NN) + (
        dot(inv_high, both_low, NN) + dot(inv_low, both_high, NN)
    )
    rhs_high, rhs_low = split2(rhs_t)
    x_t = dot(rhs_high, inv_high, NN) + (
        dot(rhs_high, inv_low, NN) + dot(rhs_low, inv_high, NN)
    )
    s_high, s_low = split2(solved)
    grams = dot(both_high, s_high, TN) + (dot(both_high, s_low, TN) + dot(both_low, s_high, TN))
    x_high, x_low = split2(x_t)
    projs = dot(x_high, both_high, NN) + (dot(x_high, both_low, NN) + dot(x_low, both_high, NN))
    shape = (2, NZ, 8, RANK)
    prod_ref[0, 0:2] = grams[:RANK, :RANK].reshape(shape)
    prod_ref[0, 2:4] = grams[:RANK, RANK:].reshape(shape)
    prod_ref[1, 0:2] = grams[RANK:, RANK:].reshape(shape)
    prod_ref[1, 2] = projs[:, :RANK].reshape(shape[1:])
    prod_ref[1, 3] = projs[:, RANK:].reshape(shape[1:])
    s_high_ref[...] = s_high
    s_low_ref[...] = s_low
    x_ref[...] = x_t


def whole_kernel(
    rhs_hbm, inv_hbm, one_hbm, two_hbm, coarse_hbm, fine_hbm, out_ref,
    s_high_ref, s_low_ref, x_ref, schur_ref, coef_ref,
    rhs_ref, inv_ref, one_ref, two_ref, buf_ref,
    prod_ref, from_core, chip_sum, from_plane, x_sum, by_y, leaving,
    work_ref, high_ref, low_ref, coarse_ref, fine_ref,
    in_s, core_s, core_r, p_s, p_r, y_s, y_r, w_s, w_r, gz_s, gz_r, gx_s, gx_r, o_s, o_r,
):
    gx, gy = lax.axis_index("gx"), lax.axis_index("gy")
    y, x_hi = lax.div(gx, 2), lax.rem(gx, 2)
    z, x_lo, core = lax.div(gy, 4), lax.rem(lax.div(gy, 2), 2), lax.rem(gy, 2)
    x = x_hi * 2 + x_lo
    other = 1 - core
    sibling = (gx, gy + 1 - 2 * core)

    def plane_peer(up, over):
        z_there, x_there = lax.rem(z + up, NZ), lax.rem(x + over, NX)
        gx_there = y * 2 + lax.div(x_there, 2)
        return z_there, x_there, (gx_there, z_there * 4 + lax.rem(x_there, 2) * 2 + core)

    def z_peer(step):
        there = lax.rem(z + step, NZ)
        return there, (gx, there * 4 + x_lo * 2 + core)

    def x_peer(step):
        there = lax.rem(x + step, NX)
        return there, (y * 2 + lax.div(there, 2), z * 4 + lax.rem(there, 2) * 2 + core)

    def y_peer(step):
        there = lax.rem(y + step, NY)
        return there, (there * 2 + x_hi, gy)

    barrier = pltpu.get_barrier_semaphore()
    peers = [plane_peer(up, over)[2] for up, over in plane_steps()]
    peers += [y_peer(step)[1] for step in farthest_first(NY)]
    peers += [sibling]
    for peer in peers:
        pl.semaphore_signal(barrier, inc=1, device_id=peer, device_id_type=MESH)

    loads = [
        pltpu.make_async_copy(source, target, in_s.at[index])
        for index, (source, target) in enumerate(
            ((inv_hbm, inv_ref), (two_hbm, two_ref), (one_hbm, one_ref), (rhs_hbm, rhs_ref),
             (fine_hbm, fine_ref), (coarse_hbm, coarse_ref))
        )
    ]
    for load in loads:
        load.start()
    for load in loads[:4]:
        load.wait()
    local_products(
        inv_ref[...], two_ref[...], one_ref[...], rhs_ref[...],
        prod_ref, s_high_ref, s_low_ref, x_ref,
    )
    pl.semaphore_wait(barrier, len(peers))

    def send(source, target, send_sem, recv_sem, peer):
        copy = pltpu.make_async_remote_copy(
            src_ref=source, dst_ref=target, send_sem=send_sem, recv_sem=recv_sem,
            device_id=peer, device_id_type=MESH,
        )
        copy.start()
        return copy

    first = send(prod_ref.at[other], from_core, core_s, core_r, sibling)
    first.wait()
    for there in range(NX):
        chip_sum[:, there] = prod_ref[core, there] + from_core[there]

    copies = []
    for up, over in plane_steps():
        z_there, x_there, peer = plane_peer(up, over)
        at = up * NX + over - 1
        copies.append(
            send(chip_sum.at[z_there, x_there], from_plane.at[at], p_s.at[at], p_r.at[at], peer)
        )
    total = chip_sum[z, x]
    for copy in copies:
        copy.wait()
    for at in range(NZ * NX - 1):
        total = total + from_plane[at]
    x_sum[...] = total

    copies = []
    for step in farthest_first(NY):
        _, peer = y_peer(step)
        copies.append(send(x_sum, by_y.at[y], y_s.at[step - 1], y_r.at[step - 1], peer))
    by_y[y] = total
    for copy in copies:
        copy.wait()
    for slab in range(2):
        here, there = core * 4 + 2 * slab, other * 4 + 2 * slab
        leaving[slab] = by_y[there] + by_y[there + 1]
        buf_ref[x, z, core, slab] = by_y[here] + by_y[here + 1]
    send(leaving, buf_ref.at[x, z, core], w_s, w_r, sibling).wait()

    copies = []
    place = buf_ref.at[x, z]
    for step in farthest_first(NZ):
        _, peer = z_peer(step)
        copies.append(send(place, place, gz_s.at[step - 1], gz_r.at[step - 1], peer))
    for copy in copies:
        copy.wait()

    waves = []
    for wave in range(2):
        place = buf_ref.at[x, :, wave]
        copies = []
        for step in farthest_first(NX):
            _, peer = x_peer(step)
            at = wave * 3 + step - 1
            copies.append(send(place, place, gx_s.at[at], gx_r.at[at], peer))
        waves.append(copies)
    for copy in waves[0]:
        copy.wait()

    for load in loads[4:]:
        load.wait()
    factor = fine_ref[core]
    cap = capacitance(factor, [part(buf_ref, 0, 0), part(buf_ref, 0, 1)])
    mixed = jnp.concatenate((part(buf_ref, 1, 0), part(buf_ref, 1, 1)), axis=0)
    coarse_term = mm_exact_left(factor, mixed, TN)
    eye = identity()
    work_ref[0] = cap[:RANK, :RANK] + eye
    invert_in_place(work_ref, high_ref, low_ref, 1)
    for copy in waves[1]:
        copy.wait()
    rights = [part(buf_ref, 3, slab) for slab in range(2)]
    right = jnp.concatenate([rights[slab][:64].T for slab in range(2)], axis=0)
    term = jnp.concatenate((coarse_term, mm_exact_left(factor, right, TN)), axis=1)
    top, low = finish_solve(cap, term, work_ref, high_ref, low_ref)
    inner = mm(term[:RANK, :RANK], top, TN) + mm(term[RANK:, :RANK], low, TN)
    coef_ref[core, :RANK] = top
    coef_ref[core, RANK:] = low
    schur_ref[core, :, :RANK] = part(buf_ref, 2, 0) + part(buf_ref, 2, 1) - inner[:, :RANK]
    schur_ref[core, :, RANK:] = (rights[0][64:] + rights[1][64:]).T - inner[:, RANK:]
    swaps = [
        send(ref.at[core], ref.at[core], o_s.at[at], o_r.at[at], sibling)
        for at, ref in enumerate((schur_ref, coef_ref))
    ]
    for swap in swaps:
        swap.wait()

    block = lax.div(gx, 4)
    my_pair, my_half = lax.div(block, 2), lax.rem(block, 2)
    factor = coarse_ref[0]
    cap = capacitance(factor, [schur_ref[0, :, :RANK], schur_ref[1, :, :RANK]])
    term = mm_exact_left(
        factor, jnp.concatenate((schur_ref[0, :, RANK:], schur_ref[1, :, RANK:]), axis=0), TN
    )
    work_ref[0] = cap[:RANK, :RANK] + identity()
    invert_in_place(work_ref, high_ref, low_ref, 1)
    top, low = finish_solve(cap, term, work_ref, high_ref, low_ref)
    half_rows = pl.ds(pl.multiple_of(my_pair * RANK, RANK), RANK)
    m1 = mm_exact_left(coarse_ref[0, half_rows, :], jnp.concatenate((top, low), axis=0))
    own = coef_ref[my_pair]
    inner = own[:, RANK:] - mm(own[:, :RANK], m1)
    block_rows = pl.ds(pl.multiple_of(my_half * RANK, RANK), RANK)
    m2 = mm_exact_left(fine_ref[my_pair, block_rows, :], inner)
    weights = jnp.concatenate((m2, m1), axis=0).T
    w_high, w_low = split2(weights)
    s_high = s_high_ref[...]
    out_ref[...] = x_ref[...] - (
        dot(w_high, s_high, NT) + (dot(w_high, s_low_ref[...], NT) + dot(w_low, s_high, NT))
    )


def row_of(tile, index):
    return jnp.broadcast_to(tile[index : index + 1, :], tile.shape)


def reciprocal(value):
    guess = pl.reciprocal(value, approx=True)
    guess = guess * (2.0 - value * guess)
    return guess * (2.0 - value * guess)


def panel_solve(tiles, cols, unit_rows):
    scale = [jnp.ones((8, RANK), F32)] * 2
    cols = [list(pair) for pair in cols]
    for k in range(16):
        at, sub = k // 8, k % 8
        inverse = reciprocal(row_of(cols[k][at], sub))
        here = unit_rows == sub
        scale[at] = jnp.where(here, inverse, scale[at])
        factors = list(cols[k])
        factors[at] = jnp.where(here, 0.0, factors[at])
        factors = [factor * inverse for factor in factors]
        for j in range(k + 1, 16):
            across = row_of(cols[j][at], sub)
            cols[j] = [cols[j][t] - factors[t] * across for t in range(2)]
        across = row_of(tiles[at], sub)
        tiles = [tiles[t] - factors[t] * across for t in range(2)]
    return [tiles[t] * scale[t] for t in range(2)]


def invert_in_place(work_ref, high_ref, low_ref, count):
    rows = lax.broadcasted_iota(jnp.int32, (8, RANK), 0)
    lanes = lax.broadcasted_iota(jnp.int32, (8, RANK), 1)
    tile_count = RANK // 8

    def apply_last(which, base_before, place, before):
        last = jnp.logical_and(lanes >= base_before, lanes < base_before + 16)
        whole = work_ref[which]
        left_high, left_low = split2(whole)
        high, low = high_ref[which], low_ref[which]
        update = dot(left_high, high, NN) + (dot(left_high, low, NN) + dot(left_low, high, NN))
        for tile in range(tile_count):
            at = slice(tile * 8, tile * 8 + 8)
            work_ref[which, at, :] = jnp.where(last, 0.0, whole[at]) - update[at]
        work_ref[which, place, :] = jnp.concatenate(before, axis=0)

    def step(panel, carry):
        base = panel * 16
        inside = jnp.logical_and(lanes >= base, lanes < base + 16)
        picks = [jnp.full((8, RANK), base + j, jnp.int32) for j in range(16)]
        following = lax.rem(base + 16, RANK)
        gone = pl.ds(pl.multiple_of(lax.rem(base + RANK - 16, RANK), 16), 16)
        after = []
        for which in range(count):
            current, before = carry[which]
            cols = [
                [jnp.take_along_axis(current[t], picks[j], axis=1) for t in range(2)]
                for j in range(16)
            ]
            tiles = [
                jnp.where(inside, (lanes - base == rows + 8 * t).astype(F32), current[t])
                for t in range(2)
            ]
            apply_last(which, base - 16, gone, before)
            solved = panel_solve(tiles, cols, rows)
            joined = jnp.concatenate(solved, axis=0)
            high, low = split2(joined)
            high_ref[which, gone, :] = jnp.zeros((16, RANK), BF16)
            low_ref[which, gone, :] = jnp.zeros((16, RANK), BF16)
            at = pl.ds(pl.multiple_of(base, 16), 16)
            high_ref[which, at, :] = high
            low_ref[which, at, :] = low
            upcoming = []
            for t in range(2):
                tile = work_ref[which, pl.ds(pl.multiple_of(following + 8 * t, 8), 8), :]
                fresh = jnp.where(inside, 0.0, tile)
                for j in range(16):
                    weight = jnp.take_along_axis(tile, picks[j], axis=1)
                    fresh = fresh - weight * row_of(solved[j // 8], j % 8)
                upcoming.append(fresh)
            after.append((tuple(upcoming), tuple(solved)))
        return tuple(after)

    start = []
    for which in range(count):
        high_ref[which] = jnp.zeros((RANK, RANK), BF16)
        low_ref[which] = jnp.zeros((RANK, RANK), BF16)
        first = (work_ref[which, :8, :], work_ref[which, 8:16, :])
        end = (work_ref[which, 112:120, :], work_ref[which, 120:128, :])
        start.append((first, end))
    done = lax.fori_loop(0, RANK // 16, step, tuple(start))
    for which in range(count):
        apply_last(which, RANK - 16, slice(RANK - 16, RANK), done[which][1])


def part(buf_ref, index, slab):
    start = (index % 2) * 2
    return buf_ref[start : start + 2, :, index // 2, slab].reshape(RANK, RANK)


def capacitance(factor, grams):
    top = mm_exact_right(grams[0], factor[:RANK])
    low = mm_exact_right(grams[1], factor[RANK:])
    return mm_exact_left(factor, jnp.concatenate((top, low), axis=0), TN)


def identity():
    down = lax.broadcasted_iota(jnp.int32, (RANK, RANK), 0)
    return (down == lax.broadcasted_iota(jnp.int32, (RANK, RANK), 1)).astype(F32)


def finish_solve(cap, term, work_ref, high_ref, low_ref):
    inverse = work_ref[0]
    cross = cap[:RANK, RANK:]
    wide = mm(inverse, cross)
    work_ref[0] = cap[RANK:, RANK:] + identity() - mm(cross, wide, TN)
    first = mm(inverse, term[:RANK])
    rest = term[RANK:] - mm(cross, first, TN)
    invert_in_place(work_ref, high_ref, low_ref, 1)
    low = mm(work_ref[0], rest)
    top = first - mm(wide, low)
    return top, low


def vmem():
    return pl.BlockSpec(memory_space=pltpu.VMEM)


def shape(*dims, kind=F32):
    return jax.ShapeDtypeStruct(dims, kind)


def inverse_scratch():
    return [
        pltpu.VMEM((1, RANK, RANK), F32),
        pltpu.VMEM((1, RANK, RANK), BF16),
        pltpu.VMEM((1, RANK, RANK), BF16),
    ]


def body(right_side, leaf_inverse, basis_one, basis_two, factor_one, factor_two):
    rows = leaf_inverse.shape[0]
    dma = pltpu.SemaphoreType.DMA
    plane = NZ * NX - 1
    hbm = pl.BlockSpec(memory_space=pltpu.HBM)
    return pl.pallas_call(
        whole_kernel,
        out_shape=shape(64, rows),
        in_specs=[hbm] * 6,
        out_specs=vmem(),
        scratch_shapes=[
            pltpu.VMEM((rows, 2 * RANK), BF16),
            pltpu.VMEM((rows, 2 * RANK), BF16),
            pltpu.VMEM((64, rows), F32),
            pltpu.VMEM((2, RANK, 192), F32),
            pltpu.VMEM((2, 2 * RANK, 192), F32),
            pltpu.VMEM((64, rows), F32),
            pltpu.VMEM((rows, rows), F32),
            pltpu.VMEM((rows, RANK), F32),
            pltpu.VMEM((rows, RANK), F32),
            pltpu.VMEM((NX, NZ, 2, 2, 8, RANK), F32),
            pltpu.VMEM((2, NX, NZ, 8, RANK), F32),
            pltpu.VMEM((NX, NZ, 8, RANK), F32),
            pltpu.VMEM((NZ, NX, 8, RANK), F32),
            pltpu.VMEM((plane, 8, RANK), F32),
            pltpu.VMEM((8, RANK), F32),
            pltpu.VMEM((NY, 8, RANK), F32),
            pltpu.VMEM((2, 8, RANK), F32),
        ] + inverse_scratch() + [
            pltpu.VMEM(factor_one.shape, BF16),
            pltpu.VMEM(factor_two.shape, BF16),
            dma((6,)), dma, dma, dma((plane,)), dma((plane,)), dma((7,)), dma((7,)),
            dma, dma, dma((7,)), dma((7,)), dma((6,)), dma((6,)), dma((2,)), dma((2,)),
        ],
        compiler_params=pltpu.CompilerParams(
            collective_id=0, has_side_effects=True, vmem_limit_bytes=62 << 20
        ),
    )(right_side.T, leaf_inverse, basis_one, basis_two, factor_one, factor_two).T


def solution(mesh):
    split = P(("gx", "gy"), None)
    return jax.shard_map(
        body, mesh=mesh, in_specs=(split, split, split, split, P(), P()),
        out_specs=split, check_vma=False,
    )
```

```python
import functools

import jax
import jax.numpy as jnp
from jax import lax
from jax.experimental import pallas as pl
from jax.experimental.pallas import tpu as pltpu
from jax.sharding import PartitionSpec as P

MESH = pl.DeviceIdType.MESH
F32 = jnp.float32
BF16 = jnp.bfloat16
RANK = 128
NZ, NX, NY = 8, 4, 8


def split2(value):
    high = value.astype(BF16)
    return high, (value - high.astype(F32)).astype(BF16)


def dot(left, right, dims):
    return lax.dot_general(left, right, (dims, ((), ())), preferred_element_type=F32)


NN = ((1,), (0,))
TN = ((0,), (0,))
NT = ((1,), (1,))


def mm(left, right, dims=NN):
    left_high, left_low = split2(left)
    right_high, right_low = split2(right)
    return dot(left_high, right_high, dims) + (
        dot(left_high, right_low, dims) + dot(left_low, right_high, dims)
    )


def mm_exact_left(left, right, dims=NN):
    right_high, right_low = split2(right)
    return dot(left, right_high, dims) + dot(left, right_low, dims)


def mm_exact_right(left, right, dims=NN):
    left_high, left_low = split2(left)
    return dot(left_high, right, dims) + dot(left_low, right, dims)


def away(step, count):
    return min(step, count - step)


def farthest_first(count):
    return sorted(range(1, count), key=lambda step: -away(step, count))


def plane_steps():
    steps = [(up, over) for up in range(NZ) for over in range(NX) if up or over]
    return sorted(steps, key=lambda step: -away(step[0], NZ) - away(step[1], NX))


def local_products(inv, two, one, rhs_t, prod_ref, s_high_ref, s_low_ref, x_ref):
    both = jnp.concatenate((two, one), axis=1)
    both_high, both_low = split2(both)
    inv_high, inv_low = split2(inv)
    solved = dot(inv_high, both_high, NN) + (
        dot(inv_high, both_low, NN) + dot(inv_low, both_high, NN)
    )
    rhs_high, rhs_low = split2(rhs_t)
    x_t = dot(rhs_high, inv_high, NN) + (
        dot(rhs_high, inv_low, NN) + dot(rhs_low, inv_high, NN)
    )
    s_high, s_low = split2(solved)
    grams = dot(both_high, s_high, TN) + (dot(both_high, s_low, TN) + dot(both_low, s_high, TN))
    x_high, x_low = split2(x_t)
    projs = dot(x_high, both_high, NN) + (dot(x_high, both_low, NN) + dot(x_low, both_high, NN))
    shape = (2, NZ, 8, RANK)
    prod_ref[0, 0:2] = grams[:RANK, :RANK].reshape(shape)
    prod_ref[0, 2:4] = grams[:RANK, RANK:].reshape(shape)
    prod_ref[1, 0:2] = grams[RANK:, RANK:].reshape(shape)
    prod_ref[1, 2] = projs[:, :RANK].reshape(shape[1:])
    prod_ref[1, 3] = projs[:, RANK:].reshape(shape[1:])
    s_high_ref[...] = s_high
    s_low_ref[...] = s_low
    x_ref[...] = x_t


def whole_kernel(
    rhs_hbm, inv_hbm, one_hbm, two_hbm, coarse_hbm, fine_hbm, out_ref,
    s_high_ref, s_low_ref, x_ref, schur_ref, coef_ref,
    rhs_ref, inv_ref, one_ref, two_ref, buf_ref,
    prod_ref, from_core, chip_sum, from_plane, x_sum, by_y, leaving,
    work_ref, high_ref, low_ref, coarse_ref, fine_ref, coarse_t, fine_t,
    in_s, core_s, core_r, p_s, p_r, y_s, y_r, w_s, w_r, gz_s, gz_r, gx_s, gx_r, o_s, o_r,
):
    gx, gy = lax.axis_index("gx"), lax.axis_index("gy")
    y, x_hi = lax.div(gx, 2), lax.rem(gx, 2)
    z, x_lo, core = lax.div(gy, 4), lax.rem(lax.div(gy, 2), 2), lax.rem(gy, 2)
    x = x_hi * 2 + x_lo
    other = 1 - core
    sibling = (gx, gy + 1 - 2 * core)

    def plane_peer(up, over):
        z_there, x_there = lax.rem(z + up, NZ), lax.rem(x + over, NX)
        gx_there = y * 2 + lax.div(x_there, 2)
        return z_there, x_there, (gx_there, z_there * 4 + lax.rem(x_there, 2) * 2 + core)

    def z_peer(step):
        there = lax.rem(z + step, NZ)
        return there, (gx, there * 4 + x_lo * 2 + core)

    def x_peer(step):
        there = lax.rem(x + step, NX)
        return there, (y * 2 + lax.div(there, 2), z * 4 + lax.rem(there, 2) * 2 + core)

    def y_peer(step):
        there = lax.rem(y + step, NY)
        return there, (there * 2 + x_hi, gy)

    loads = [
        pltpu.make_async_copy(source, target, in_s.at[index])
        for index, (source, target) in enumerate(
            ((inv_hbm, inv_ref), (two_hbm, two_ref), (one_hbm, one_ref), (rhs_hbm, rhs_ref),
             (fine_hbm, fine_ref), (coarse_hbm, coarse_ref))
        )
    ]
    for load in loads:
        load.start()

    barrier = pltpu.get_barrier_semaphore()
    peers = [plane_peer(up, over)[2] for up, over in plane_steps()]
    peers += [y_peer(step)[1] for step in farthest_first(NY)]
    peers += [sibling]
    for peer in peers:
        pl.semaphore_signal(barrier, inc=1, device_id=peer, device_id_type=MESH)

    for load in loads[:4]:
        load.wait()
    local_products(
        inv_ref[...], two_ref[...], one_ref[...], rhs_ref[...],
        prod_ref, s_high_ref, s_low_ref, x_ref,
    )
    pl.semaphore_wait(barrier, len(peers))

    def send(source, target, send_sem, recv_sem, peer):
        copy = pltpu.make_async_remote_copy(
            src_ref=source, dst_ref=target, send_sem=send_sem, recv_sem=recv_sem,
            device_id=peer, device_id_type=MESH,
        )
        copy.start()
        return copy

    first = send(prod_ref.at[other], from_core, core_s, core_r, sibling)
    first.wait()
    for there in range(NX):
        chip_sum[:, there] = prod_ref[core, there] + from_core[there]

    copies = []
    for up, over in plane_steps():
        z_there, x_there, peer = plane_peer(up, over)
        at = up * NX + over - 1
        copies.append(
            send(chip_sum.at[z_there, x_there], from_plane.at[at], p_s.at[at], p_r.at[at], peer)
        )
    for load in loads[4:]:
        load.wait()
    fine_t[...] = fine_ref[core].T
    coarse_t[...] = coarse_ref[0].T
    total = chip_sum[z, x]
    for copy in copies:
        copy.wait()
    for at in range(NZ * NX - 1):
        total = total + from_plane[at]
    x_sum[...] = total

    copies = []
    for step in farthest_first(NY):
        _, peer = y_peer(step)
        copies.append(send(x_sum, by_y.at[y], y_s.at[step - 1], y_r.at[step - 1], peer))
    by_y[y] = total
    for copy in copies:
        copy.wait()
    for slab in range(2):
        here, there = core * 4 + 2 * slab, other * 4 + 2 * slab
        leaving[slab] = by_y[there] + by_y[there + 1]
        buf_ref[x, z, core, slab] = by_y[here] + by_y[here + 1]
    send(leaving, buf_ref.at[x, z, core], w_s, w_r, sibling).wait()

    copies = []
    place = buf_ref.at[x, z]
    for step in farthest_first(NZ):
        _, peer = z_peer(step)
        copies.append(send(place, place, gz_s.at[step - 1], gz_r.at[step - 1], peer))
    for copy in copies:
        copy.wait()

    waves = []
    for wave in range(2):
        place = buf_ref.at[x, :, wave]
        copies = []
        for step in farthest_first(NX):
            _, peer = x_peer(step)
            at = wave * 3 + step - 1
            copies.append(send(place, place, gx_s.at[at], gx_r.at[at], peer))
        waves.append(copies)
    for copy in waves[0]:
        copy.wait()

    factor, factor_t = fine_ref[core], fine_t[...]
    cap = capacitance(factor, factor_t, [part(buf_ref, 0, 0), part(buf_ref, 0, 1)])
    mixed = jnp.concatenate((part(buf_ref, 1, 0), part(buf_ref, 1, 1)), axis=0)
    coarse_term = mm_exact_left(factor_t, mixed)
    eye = identity()
    work_ref[0] = cap[:RANK, :RANK] + eye
    invert_in_place(work_ref, high_ref, low_ref, 1)
    for copy in waves[1]:
        copy.wait()
    rights = [part(buf_ref, 3, slab) for slab in range(2)]
    right = jnp.concatenate([rights[slab][:64].T for slab in range(2)], axis=0)
    term = jnp.concatenate((coarse_term, mm_exact_left(factor_t, right)), axis=1)
    top, low = finish_solve(cap, term, work_ref, high_ref, low_ref)
    inner = mm(term[:RANK, :RANK], top, TN) + mm(term[RANK:, :RANK], low, TN)
    coef_ref[core] = mm_exact_left(factor, jnp.concatenate((top, low), axis=0))
    schur_ref[core, :, :RANK] = part(buf_ref, 2, 0) + part(buf_ref, 2, 1) - inner[:, :RANK]
    schur_ref[core, :, RANK:] = (rights[0][64:] + rights[1][64:]).T - inner[:, RANK:]
    swaps = [
        send(ref.at[core], ref.at[core], o_s.at[at], o_r.at[at], sibling)
        for at, ref in enumerate((schur_ref, coef_ref))
    ]
    for swap in swaps:
        swap.wait()

    block = lax.div(gx, 4)
    my_pair, my_half = lax.div(block, 2), lax.rem(block, 2)
    factor = coarse_ref[0]
    factor_t = coarse_t[...]
    cap = capacitance(factor, factor_t, [schur_ref[0, :, :RANK], schur_ref[1, :, :RANK]])
    term = mm_exact_left(
        factor_t, jnp.concatenate((schur_ref[0, :, RANK:], schur_ref[1, :, RANK:]), axis=0)
    )
    work_ref[0] = cap[:RANK, :RANK] + identity()
    invert_in_place(work_ref, high_ref, low_ref, 1)
    top, low = finish_solve(cap, term, work_ref, high_ref, low_ref)
    half_rows = pl.ds(pl.multiple_of(my_pair * RANK, RANK), RANK)
    m1 = mm_exact_left(coarse_ref[0, half_rows, :], jnp.concatenate((top, low), axis=0))
    own = coef_ref[my_pair, pl.ds(pl.multiple_of(my_half * RANK, RANK), RANK), :]
    m2 = own[:, RANK:] - mm(own[:, :RANK], m1)
    weights = jnp.concatenate((m2, m1), axis=0).T
    w_high, w_low = split2(weights)
    s_high = s_high_ref[...]
    out_ref[...] = x_ref[...] - (
        dot(w_high, s_high, NT) + (dot(w_high, s_low_ref[...], NT) + dot(w_low, s_high, NT))
    )


def row_of(tile, index):
    return jnp.broadcast_to(tile[index : index + 1, :], tile.shape)


def spread(tile, pick):
    column = jnp.sum(jnp.where(pick, tile, 0.0), axis=1, keepdims=True)
    return jnp.broadcast_to(column, tile.shape)


def combine(weights, solved):
    sums = [jnp.zeros((8, RANK), F32)] * 4
    for j in range(16):
        sums[j % 4] = sums[j % 4] + weights[j] * row_of(solved[j // 8], j % 8)
    return (sums[0] + sums[1]) + (sums[2] + sums[3])


def panel_solve(tiles, cols, rows):
    scale = [jnp.ones((8, RANK), F32)] * 2
    cols = [list(pair) for pair in cols]
    for k in range(16):
        at, sub = k // 8, k % 8
        pivot = row_of(cols[k][at], sub)
        guess = pl.reciprocal(pivot, approx=True)
        refine = 2.0 - pivot * guess
        inverse = guess * refine
        here = rows == sub
        scale[at] = jnp.where(here, inverse, scale[at])
        raw = list(cols[k])
        raw[at] = jnp.where(here, 0.0, raw[at])
        factors = [value * inverse for value in raw]
        for j in range(k + 1, 16):
            across = row_of(cols[j][at], sub)
            if j == k + 1:
                cols[j] = [cols[j][t] - (raw[t] * across * guess) * refine for t in range(2)]
            else:
                cols[j] = [cols[j][t] - factors[t] * across for t in range(2)]
        across = row_of(tiles[at], sub)
        tiles = [tiles[t] - factors[t] * across for t in range(2)]
    return [tiles[t] * scale[t] for t in range(2)]


def invert_in_place(work_ref, high_ref, low_ref, count):
    rows = lax.broadcasted_iota(jnp.int32, (8, RANK), 0)
    lanes = lax.broadcasted_iota(jnp.int32, (8, RANK), 1)
    tile_count = RANK // 8

    def apply_last(which, base_before, place, before):
        last = jnp.logical_and(lanes >= base_before, lanes < base_before + 16)
        whole = work_ref[which]
        left_high, left_low = split2(whole)
        high, low = high_ref[which], low_ref[which]
        update = dot(left_high, high, NN) + (dot(left_high, low, NN) + dot(left_low, high, NN))
        for tile in range(tile_count):
            at = slice(tile * 8, tile * 8 + 8)
            work_ref[which, at, :] = jnp.where(last, 0.0, whole[at]) - update[at]
        work_ref[which, place, :] = jnp.concatenate(before, axis=0)

    def step(panel, carry):
        base = panel * 16
        inside = jnp.logical_and(lanes >= base, lanes < base + 16)
        earlier = jnp.logical_and(lanes >= base - 16, lanes < base)
        picks = [lanes == base + j for j in range(16)]
        last_picks = [lanes == base - 16 + j for j in range(16)]
        following = lax.rem(base + 32, RANK)
        gone = pl.ds(pl.multiple_of(lax.rem(base + RANK - 16, RANK), 16), 16)
        after = []
        for which in range(count):
            current, coming, before = carry[which]
            old = [[spread(tile, pick) for pick in last_picks] for tile in coming]
            coming = [
                jnp.where(earlier, 0.0, coming[t]) - combine(old[t], before) for t in range(2)
            ]
            weights = [[spread(tile, pick) for pick in picks] for tile in coming]
            cols = [
                [spread(current[t], picks[j]) for t in range(2)]
                for j in range(16)
            ]
            tiles = [
                jnp.where(inside, (lanes - base == rows + 8 * t).astype(F32), current[t])
                for t in range(2)
            ]
            apply_last(which, base - 16, gone, before)
            solved = panel_solve(tiles, cols, rows)
            joined = jnp.concatenate(solved, axis=0)
            high, low = split2(joined)
            high_ref[which, gone, :] = jnp.zeros((16, RANK), BF16)
            low_ref[which, gone, :] = jnp.zeros((16, RANK), BF16)
            at = pl.ds(pl.multiple_of(base, 16), 16)
            high_ref[which, at, :] = high
            low_ref[which, at, :] = low
            upcoming = [
                jnp.where(inside, 0.0, coming[t]) - combine(weights[t], solved) for t in range(2)
            ]
            stale = [
                work_ref[which, pl.ds(pl.multiple_of(following + 8 * t, 8), 8), :] for t in range(2)
            ]
            after.append((tuple(upcoming), tuple(stale), tuple(solved)))
        return tuple(after)

    start = []
    for which in range(count):
        high_ref[which] = jnp.zeros((RANK, RANK), BF16)
        low_ref[which] = jnp.zeros((RANK, RANK), BF16)
        first = (work_ref[which, :8, :], work_ref[which, 8:16, :])
        end = (work_ref[which, 112:120, :], work_ref[which, 120:128, :])
        second = (work_ref[which, 16:24, :], work_ref[which, 24:32, :])
        start.append((first, second, end))
    done = lax.fori_loop(0, RANK // 16, step, tuple(start))
    for which in range(count):
        apply_last(which, RANK - 16, slice(RANK - 16, RANK), done[which][2])


def part(buf_ref, index, slab):
    start = (index % 2) * 2
    return buf_ref[start : start + 2, :, index // 2, slab].reshape(RANK, RANK)


def capacitance(factor, factor_t, grams):
    top = mm_exact_right(grams[0], factor[:RANK])
    low = mm_exact_right(grams[1], factor[RANK:])
    return mm_exact_left(factor_t, jnp.concatenate((top, low), axis=0))


def identity():
    down = lax.broadcasted_iota(jnp.int32, (RANK, RANK), 0)
    return (down == lax.broadcasted_iota(jnp.int32, (RANK, RANK), 1)).astype(F32)


def finish_solve(cap, term, work_ref, high_ref, low_ref):
    inverse = work_ref[0]
    wide = mm(inverse, cap[:RANK, RANK:])
    cross = cap[RANK:, :RANK]
    work_ref[0] = cap[RANK:, RANK:] + identity() - mm(cross, wide)
    first = mm(inverse, term[:RANK])
    rest = term[RANK:] - mm(cross, first)
    invert_in_place(work_ref, high_ref, low_ref, 1)
    low = mm(work_ref[0], rest)
    top = first - mm(wide, low)
    return top, low


def vmem():
    return pl.BlockSpec(memory_space=pltpu.VMEM)


def shape(*dims, kind=F32):
    return jax.ShapeDtypeStruct(dims, kind)


def inverse_scratch():
    return [
        pltpu.VMEM((1, RANK, RANK), F32),
        pltpu.VMEM((1, RANK, RANK), BF16),
        pltpu.VMEM((1, RANK, RANK), BF16),
    ]


def body(right_side, leaf_inverse, basis_one, basis_two, factor_one, factor_two):
    rows = leaf_inverse.shape[0]
    dma = pltpu.SemaphoreType.DMA
    plane = NZ * NX - 1
    hbm = pl.BlockSpec(memory_space=pltpu.HBM)
    return pl.pallas_call(
        whole_kernel,
        out_shape=shape(64, rows),
        in_specs=[hbm] * 6,
        out_specs=vmem(),
        scratch_shapes=[
            pltpu.VMEM((rows, 2 * RANK), BF16),
            pltpu.VMEM((rows, 2 * RANK), BF16),
            pltpu.VMEM((64, rows), F32),
            pltpu.VMEM((2, RANK, 192), F32),
            pltpu.VMEM((2, 2 * RANK, 192), F32),
            pltpu.VMEM((64, rows), F32),
            pltpu.VMEM((rows, rows), F32),
            pltpu.VMEM((rows, RANK), F32),
            pltpu.VMEM((rows, RANK), F32),
            pltpu.VMEM((NX, NZ, 2, 2, 8, RANK), F32),
            pltpu.VMEM((2, NX, NZ, 8, RANK), F32),
            pltpu.VMEM((NX, NZ, 8, RANK), F32),
            pltpu.VMEM((NZ, NX, 8, RANK), F32),
            pltpu.VMEM((plane, 8, RANK), F32),
            pltpu.VMEM((8, RANK), F32),
            pltpu.VMEM((NY, 8, RANK), F32),
            pltpu.VMEM((2, 8, RANK), F32),
        ] + inverse_scratch() + [
            pltpu.VMEM(factor_one.shape, BF16),
            pltpu.VMEM(factor_two.shape, BF16),
            pltpu.VMEM((2 * RANK, 2 * RANK), BF16),
            pltpu.VMEM((2 * RANK, 2 * RANK), BF16),
            dma((6,)), dma, dma, dma((plane,)), dma((plane,)), dma((7,)), dma((7,)),
            dma, dma, dma((7,)), dma((7,)), dma((6,)), dma((6,)), dma((2,)), dma((2,)),
        ],
        compiler_params=pltpu.CompilerParams(
            collective_id=0, has_side_effects=True, vmem_limit_bytes=62 << 20
        ),
    )(right_side.T, leaf_inverse, basis_one, basis_two, factor_one, factor_two).T


def solution(mesh):
    split = P(("gx", "gy"), None)
    return jax.shard_map(
        body, mesh=mesh, in_specs=(split, split, split, split, P(), P()),
        out_specs=split, check_vma=False,
    )
```

```python
import functools

import jax
import jax.numpy as jnp
from jax import lax
from jax.experimental import pallas as pl
from jax.experimental.pallas import tpu as pltpu
from jax.sharding import PartitionSpec as P

MESH = pl.DeviceIdType.MESH
F32 = jnp.float32
BF16 = jnp.bfloat16
RANK = 128
NZ, NX, NY = 8, 4, 8


def split2(value):
    high = value.astype(BF16)
    return high, (value - high.astype(F32)).astype(BF16)


def dot(left, right, dims):
    return lax.dot_general(left, right, (dims, ((), ())), preferred_element_type=F32)


NN = ((1,), (0,))
TN = ((0,), (0,))
NT = ((1,), (1,))


def mm(left, right, dims=NN):
    left_high, left_low = split2(left)
    right_high, right_low = split2(right)
    return dot(left_high, right_high, dims) + (
        dot(left_high, right_low, dims) + dot(left_low, right_high, dims)
    )


def mm_exact_left(left, right, dims=NN):
    right_high, right_low = split2(right)
    return dot(left, right_high, dims) + dot(left, right_low, dims)


def mm_exact_right(left, right, dims=NN):
    left_high, left_low = split2(left)
    return dot(left_high, right, dims) + dot(left_low, right, dims)


def away(step, count):
    return min(step, count - step)


def farthest_first(count):
    return sorted(range(1, count), key=lambda step: -away(step, count))


def plane_steps():
    steps = [(up, over) for up in range(NZ) for over in range(NX) if up or over]
    return sorted(steps, key=lambda step: -away(step[0], NZ) - away(step[1], NX))


def local_products(inv, two, one, rhs_t, prod_ref, s_high_ref, s_low_ref, x_ref):
    both = jnp.concatenate((two, one), axis=1)
    both_high, both_low = split2(both)
    inv_high, inv_low = split2(inv)
    solved = dot(inv_high, both_high, NN) + (
        dot(inv_high, both_low, NN) + dot(inv_low, both_high, NN)
    )
    rhs_high, rhs_low = split2(rhs_t)
    x_t = dot(rhs_high, inv_high, NN) + (
        dot(rhs_high, inv_low, NN) + dot(rhs_low, inv_high, NN)
    )
    s_high, s_low = split2(solved)
    grams = dot(both_high, s_high, TN) + (dot(both_high, s_low, TN) + dot(both_low, s_high, TN))
    x_high, x_low = split2(x_t)
    projs = dot(x_high, both_high, NN) + (dot(x_high, both_low, NN) + dot(x_low, both_high, NN))
    shape = (NX, NZ // 2, 8, RANK)
    prod_ref[0, :, :4] = grams[:RANK, :RANK].reshape(shape)
    prod_ref[0, :, 4:] = grams[:RANK, RANK:].reshape(shape)
    prod_ref[1, :, :4] = grams[RANK:, RANK:].reshape(shape)
    prod_ref[1, :2, 4:] = projs[:, :RANK].reshape(2, NZ // 2, 8, RANK)
    prod_ref[1, 2:, 4:] = projs[:, RANK:].reshape(2, NZ // 2, 8, RANK)
    s_high_ref[...] = s_high
    s_low_ref[...] = s_low
    x_ref[...] = x_t


def whole_kernel(
    rhs_hbm, inv_hbm, one_hbm, two_hbm, coarse_hbm, fine_hbm, out_ref,
    s_high_ref, s_low_ref, x_ref, schur_ref, coef_ref,
    rhs_ref, inv_ref, one_ref, two_ref, buf_ref,
    prod_ref, from_core, chip_sum, from_plane, x_sum, by_y,
    work_ref, high_ref, low_ref, coarse_ref, fine_ref, coarse_t, fine_t,
    in_s, core_s, core_r, p_s, p_r, y_s, y_r, gz_s, gz_r, gx_s, gx_r, o_s, o_r,
):
    gx, gy = lax.axis_index("gx"), lax.axis_index("gy")
    y, x_hi = lax.div(gx, 2), lax.rem(gx, 2)
    z, x_lo, core = lax.div(gy, 4), lax.rem(lax.div(gy, 2), 2), lax.rem(gy, 2)
    x = x_hi * 2 + x_lo
    other, solver = 1 - core, lax.div(y, 4)
    sibling = (gx, gy + 1 - 2 * core)

    def plane_peer(up, over):
        z_there, x_there = lax.rem(z + up, NZ), lax.rem(x + over, NX)
        gx_there = y * 2 + lax.div(x_there, 2)
        return z_there, x_there, (gx_there, z_there * 4 + lax.rem(x_there, 2) * 2 + core)

    def z_peer(step):
        there = lax.rem(z + step, NZ)
        return there, (gx, there * 4 + x_lo * 2 + core)

    def x_peer(step):
        there = lax.rem(x + step, NX)
        return there, (y * 2 + lax.div(there, 2), z * 4 + lax.rem(there, 2) * 2 + core)

    loads = [
        pltpu.make_async_copy(source, target, in_s.at[index])
        for index, (source, target) in enumerate(
            ((inv_hbm, inv_ref), (two_hbm, two_ref), (one_hbm, one_ref), (rhs_hbm, rhs_ref),
             (fine_hbm, fine_ref), (coarse_hbm, coarse_ref))
        )
    ]
    for load in loads:
        load.start()

    barrier = pltpu.get_barrier_semaphore()
    peers = [plane_peer(up, over)[2] for up, over in plane_steps()]
    for step in farthest_first(NY):
        there = lax.rem(y + step, NY)
        for which in range(2):
            peers.append((there * 2 + x_hi, z * 4 + x_lo * 2 + which))
    peers += [sibling]
    for peer in peers:
        pl.semaphore_signal(barrier, inc=1, device_id=peer, device_id_type=MESH)

    for load in loads[:4]:
        load.wait()
    local_products(
        inv_ref[...], two_ref[...], one_ref[...], rhs_ref[...],
        prod_ref, s_high_ref, s_low_ref, x_ref,
    )
    pl.semaphore_wait(barrier, len(peers))

    def send(source, target, send_sem, recv_sem, peer):
        copy = pltpu.make_async_remote_copy(
            src_ref=source, dst_ref=target, send_sem=send_sem, recv_sem=recv_sem,
            device_id=peer, device_id_type=MESH,
        )
        copy.start()
        return copy

    first = send(prod_ref.at[other], from_core, core_s, core_r, sibling)
    first.wait()
    for there in range(NX):
        chip_sum[:, there] = prod_ref[core, there] + from_core[there]

    copies = []
    for up, over in plane_steps():
        z_there, x_there, peer = plane_peer(up, over)
        at = up * NX + over - 1
        copies.append(
            send(chip_sum.at[z_there, x_there], from_plane.at[at], p_s.at[at], p_r.at[at], peer)
        )
    for load in loads[4:]:
        load.wait()
    fine_t[...] = fine_ref[core].T
    coarse_t[...] = coarse_ref[0].T
    total = chip_sum[z, x]
    for copy in copies:
        copy.wait()
    for at in range(NZ * NX - 1):
        total = total + from_plane[at]
    x_sum[...] = total

    copies = []
    own = lax.rem(y, 4) * 2 + core
    slot = by_y.at[lax.rem(y, 4), core]
    for step in farthest_first(NY):
        there = lax.rem(y + step, NY)
        peer = (there * 2 + x_hi, z * 4 + x_lo * 2 + solver)
        copies.append(send(x_sum, slot, y_s.at[step - 1], y_r.at[own], peer))

    @pl.when(solver == core)
    def _():
        by_y[lax.rem(y, 4), core] = total

    @pl.when(solver != core)
    def _():
        send(x_sum, slot, y_s.at[7], y_r.at[own], sibling).wait_send()

    for copy in copies:
        copy.wait_send()
    for at in range(8):
        @pl.when(jnp.logical_not(jnp.logical_and(solver == core, own == at)))
        def _():
            pltpu.make_async_remote_copy(
                src_ref=x_sum, dst_ref=by_y.at[at // 2, at % 2], send_sem=y_s.at[0],
                recv_sem=y_r.at[at], device_id=sibling, device_id_type=MESH,
            ).wait_recv()

    for half in range(2):
        for slab in range(2):
            buf_ref[x, z, half, slab] = by_y[2 * slab, half] + by_y[2 * slab + 1, half]

    copies = []
    place = buf_ref.at[x, z]
    for step in farthest_first(NZ):
        _, peer = z_peer(step)
        copies.append(send(place, place, gz_s.at[step - 1], gz_r.at[step - 1], peer))
    for copy in copies:
        copy.wait()

    waves = []
    for wave, (first_z, count_z, half) in enumerate(((0, 4, 0), (4, 4, 0), (0, NZ, 1))):
        place = buf_ref.at[x, pl.ds(first_z, count_z), half]
        copies = []
        for step in farthest_first(NX):
            _, peer = x_peer(step)
            at = wave * 3 + step - 1
            copies.append(send(place, place, gx_s.at[at], gx_r.at[at], peer))
        waves.append(copies)
    for copy in waves[0]:
        copy.wait()

    factor, factor_t = fine_ref[core], fine_t[...]
    cap = capacitance(factor, factor_t, [part(buf_ref, 0, 0), part(buf_ref, 0, 1)])
    eye = identity()
    work_ref[0] = cap[:RANK, :RANK] + eye
    invert_in_place(work_ref, high_ref, low_ref, 1)
    for copy in waves[1] + waves[2]:
        copy.wait()
    mixed = jnp.concatenate((part(buf_ref, 1, 0), part(buf_ref, 1, 1)), axis=0)
    coarse_term = mm_exact_left(factor_t, mixed)
    rights = [part(buf_ref, 3, slab) for slab in range(2)]
    right = jnp.concatenate([rights[slab][:64].T for slab in range(2)], axis=0)
    term = jnp.concatenate((coarse_term, mm_exact_left(factor_t, right)), axis=1)
    top, low = finish_solve(cap, term, work_ref, high_ref, low_ref)
    inner = mm(term[:RANK, :RANK], top, TN) + mm(term[RANK:, :RANK], low, TN)
    coef_ref[core] = mm_exact_left(factor, jnp.concatenate((top, low), axis=0))
    schur_ref[core, :, :RANK] = part(buf_ref, 2, 0) + part(buf_ref, 2, 1) - inner[:, :RANK]
    schur_ref[core, :, RANK:] = (rights[0][64:] + rights[1][64:]).T - inner[:, RANK:]
    swaps = [
        send(ref.at[core], ref.at[core], o_s.at[at], o_r.at[at], sibling)
        for at, ref in enumerate((schur_ref, coef_ref))
    ]
    for swap in swaps:
        swap.wait()

    block = lax.div(gx, 4)
    my_pair, my_half = lax.div(block, 2), lax.rem(block, 2)
    factor = coarse_ref[0]
    factor_t = coarse_t[...]
    cap = capacitance(factor, factor_t, [schur_ref[0, :, :RANK], schur_ref[1, :, :RANK]])
    term = mm_exact_left(
        factor_t, jnp.concatenate((schur_ref[0, :, RANK:], schur_ref[1, :, RANK:]), axis=0)
    )
    work_ref[0] = cap[:RANK, :RANK] + identity()
    invert_in_place(work_ref, high_ref, low_ref, 1)
    top, low = finish_solve(cap, term, work_ref, high_ref, low_ref)
    half_rows = pl.ds(pl.multiple_of(my_pair * RANK, RANK), RANK)
    m1 = mm_exact_left(coarse_ref[0, half_rows, :], jnp.concatenate((top, low), axis=0))
    own = coef_ref[my_pair, pl.ds(pl.multiple_of(my_half * RANK, RANK), RANK), :]
    m2 = own[:, RANK:] - mm(own[:, :RANK], m1)
    weights = jnp.concatenate((m2, m1), axis=0).T
    w_high, w_low = split2(weights)
    s_high = s_high_ref[...]
    out_ref[...] = x_ref[...] - (
        dot(w_high, s_high, NT) + (dot(w_high, s_low_ref[...], NT) + dot(w_low, s_high, NT))
    )


def row_of(tile, index):
    return jnp.broadcast_to(tile[index : index + 1, :], tile.shape)


def spread(tile, pick):
    column = jnp.sum(jnp.where(pick, tile, 0.0), axis=1, keepdims=True)
    return jnp.broadcast_to(column, tile.shape)


def combine(weights, solved):
    sums = [jnp.zeros((8, RANK), F32)] * 4
    for j in range(16):
        sums[j % 4] = sums[j % 4] + weights[j] * row_of(solved[j // 8], j % 8)
    return (sums[0] + sums[1]) + (sums[2] + sums[3])


def panel_solve(tiles, cols, rows):
    scale = [jnp.ones((8, RANK), F32)] * 2
    cols = [list(pair) for pair in cols]
    for k in range(16):
        at, sub = k // 8, k % 8
        pivot = row_of(cols[k][at], sub)
        guess = pl.reciprocal(pivot, approx=True)
        refine = 2.0 - pivot * guess
        inverse = guess * refine
        here = rows == sub
        scale[at] = jnp.where(here, inverse, scale[at])
        raw = list(cols[k])
        raw[at] = jnp.where(here, 0.0, raw[at])
        factors = [value * inverse for value in raw]
        for j in range(k + 1, 16):
            across = row_of(cols[j][at], sub)
            if j == k + 1:
                cols[j] = [cols[j][t] - (raw[t] * across * guess) * refine for t in range(2)]
            else:
                cols[j] = [cols[j][t] - factors[t] * across for t in range(2)]
        across = row_of(tiles[at], sub)
        tiles = [tiles[t] - factors[t] * across for t in range(2)]
    return [tiles[t] * scale[t] for t in range(2)]


def invert_in_place(work_ref, high_ref, low_ref, count):
    rows = lax.broadcasted_iota(jnp.int32, (8, RANK), 0)
    lanes = lax.broadcasted_iota(jnp.int32, (8, RANK), 1)
    tile_count = RANK // 8

    def apply_last(which, base_before, place, before):
        last = jnp.logical_and(lanes >= base_before, lanes < base_before + 16)
        whole = work_ref[which]
        left_high, left_low = split2(whole)
        high, low = high_ref[which], low_ref[which]
        update = dot(left_high, high, NN) + (dot(left_high, low, NN) + dot(left_low, high, NN))
        for tile in range(tile_count):
            at = slice(tile * 8, tile * 8 + 8)
            work_ref[which, at, :] = jnp.where(last, 0.0, whole[at]) - update[at]
        work_ref[which, place, :] = jnp.concatenate(before, axis=0)

    def step(panel, carry):
        base = panel * 16
        inside = jnp.logical_and(lanes >= base, lanes < base + 16)
        earlier = jnp.logical_and(lanes >= base - 16, lanes < base)
        picks = [lanes == base + j for j in range(16)]
        last_picks = [lanes == base - 16 + j for j in range(16)]
        following = lax.rem(base + 32, RANK)
        gone = pl.ds(pl.multiple_of(lax.rem(base + RANK - 16, RANK), 16), 16)
        after = []
        for which in range(count):
            current, coming, before = carry[which]
            old = [[spread(tile, pick) for pick in last_picks] for tile in coming]
            coming = [
                jnp.where(earlier, 0.0, coming[t]) - combine(old[t], before) for t in range(2)
            ]
            weights = [[spread(tile, pick) for pick in picks] for tile in coming]
            cols = [
                [spread(current[t], picks[j]) for t in range(2)]
                for j in range(16)
            ]
            tiles = [
                jnp.where(inside, (lanes - base == rows + 8 * t).astype(F32), current[t])
                for t in range(2)
            ]
            apply_last(which, base - 16, gone, before)
            solved = panel_solve(tiles, cols, rows)
            joined = jnp.concatenate(solved, axis=0)
            high, low = split2(joined)
            high_ref[which, gone, :] = jnp.zeros((16, RANK), BF16)
            low_ref[which, gone, :] = jnp.zeros((16, RANK), BF16)
            at = pl.ds(pl.multiple_of(base, 16), 16)
            high_ref[which, at, :] = high
            low_ref[which, at, :] = low
            upcoming = [
                jnp.where(inside, 0.0, coming[t]) - combine(weights[t], solved) for t in range(2)
            ]
            stale = [
                work_ref[which, pl.ds(pl.multiple_of(following + 8 * t, 8), 8), :] for t in range(2)
            ]
            after.append((tuple(upcoming), tuple(stale), tuple(solved)))
        return tuple(after)

    start = []
    for which in range(count):
        high_ref[which] = jnp.zeros((RANK, RANK), BF16)
        low_ref[which] = jnp.zeros((RANK, RANK), BF16)
        first = (work_ref[which, :8, :], work_ref[which, 8:16, :])
        end = (work_ref[which, 112:120, :], work_ref[which, 120:128, :])
        second = (work_ref[which, 16:24, :], work_ref[which, 24:32, :])
        start.append((first, second, end))
    done = lax.fori_loop(0, RANK // 16, step, tuple(start))
    for which in range(count):
        apply_last(which, RANK - 16, slice(RANK - 16, RANK), done[which][2])


def part(buf_ref, index, slab):
    start = (index % 2) * 4
    return buf_ref[:, start : start + 4, index // 2, slab].reshape(RANK, RANK)


def capacitance(factor, factor_t, grams):
    top = mm_exact_right(grams[0], factor[:RANK])
    low = mm_exact_right(grams[1], factor[RANK:])
    return mm_exact_left(factor_t, jnp.concatenate((top, low), axis=0))


def identity():
    down = lax.broadcasted_iota(jnp.int32, (RANK, RANK), 0)
    return (down == lax.broadcasted_iota(jnp.int32, (RANK, RANK), 1)).astype(F32)


def finish_solve(cap, term, work_ref, high_ref, low_ref):
    inverse = work_ref[0]
    wide = mm(inverse, cap[:RANK, RANK:])
    cross = cap[RANK:, :RANK]
    work_ref[0] = cap[RANK:, RANK:] + identity() - mm(cross, wide)
    first = mm(inverse, term[:RANK])
    rest = term[RANK:] - mm(cross, first)
    invert_in_place(work_ref, high_ref, low_ref, 1)
    low = mm(work_ref[0], rest)
    top = first - mm(wide, low)
    return top, low


def vmem():
    return pl.BlockSpec(memory_space=pltpu.VMEM)


def shape(*dims, kind=F32):
    return jax.ShapeDtypeStruct(dims, kind)


def inverse_scratch():
    return [
        pltpu.VMEM((1, RANK, RANK), F32),
        pltpu.VMEM((1, RANK, RANK), BF16),
        pltpu.VMEM((1, RANK, RANK), BF16),
    ]


def body(right_side, leaf_inverse, basis_one, basis_two, factor_one, factor_two):
    rows = leaf_inverse.shape[0]
    dma = pltpu.SemaphoreType.DMA
    plane = NZ * NX - 1
    hbm = pl.BlockSpec(memory_space=pltpu.HBM)
    return pl.pallas_call(
        whole_kernel,
        out_shape=shape(64, rows),
        in_specs=[hbm] * 6,
        out_specs=vmem(),
        scratch_shapes=[
            pltpu.VMEM((rows, 2 * RANK), BF16),
            pltpu.VMEM((rows, 2 * RANK), BF16),
            pltpu.VMEM((64, rows), F32),
            pltpu.VMEM((2, RANK, 192), F32),
            pltpu.VMEM((2, 2 * RANK, 192), F32),
            pltpu.VMEM((64, rows), F32),
            pltpu.VMEM((rows, rows), F32),
            pltpu.VMEM((rows, RANK), F32),
            pltpu.VMEM((rows, RANK), F32),
            pltpu.VMEM((NX, NZ, 2, 2, 8, RANK), F32),
            pltpu.VMEM((2, NX, NZ, 8, RANK), F32),
            pltpu.VMEM((NX, NZ, 8, RANK), F32),
            pltpu.VMEM((NZ, NX, 8, RANK), F32),
            pltpu.VMEM((plane, 8, RANK), F32),
            pltpu.VMEM((8, RANK), F32),
            pltpu.VMEM((4, 2, 8, RANK), F32),
        ] + inverse_scratch() + [
            pltpu.VMEM(factor_one.shape, BF16),
            pltpu.VMEM(factor_two.shape, BF16),
            pltpu.VMEM((2 * RANK, 2 * RANK), BF16),
            pltpu.VMEM((2 * RANK, 2 * RANK), BF16),
            dma((6,)), dma, dma, dma((plane,)), dma((plane,)), dma((8,)), dma((8,)),
            dma((7,)), dma((7,)), dma((9,)), dma((9,)), dma((2,)), dma((2,)),
        ],
        compiler_params=pltpu.CompilerParams(
            collective_id=0, has_side_effects=True, vmem_limit_bytes=56_400_000
        ),
    )(right_side.T, leaf_inverse, basis_one, basis_two, factor_one, factor_two).T


def solution(mesh):
    split = P(("gx", "gy"), None)
    return jax.shard_map(
        body, mesh=mesh, in_specs=(split, split, split, split, P(), P()),
        out_specs=split, check_vma=False,
    )
```

```python
import functools

import jax
import jax.numpy as jnp
from jax import lax
from jax.experimental import pallas as pl
from jax.experimental.pallas import tpu as pltpu
from jax.sharding import PartitionSpec as P

MESH = pl.DeviceIdType.MESH
F32 = jnp.float32
BF16 = jnp.bfloat16
RANK = 128
NZ, NX, NY = 8, 4, 8


def split2(value):
    high = value.astype(BF16)
    return high, (value - high.astype(F32)).astype(BF16)


def dot(left, right, dims):
    return lax.dot_general(left, right, (dims, ((), ())), preferred_element_type=F32)


NN = ((1,), (0,))
TN = ((0,), (0,))
NT = ((1,), (1,))


def mm(left, right, dims=NN):
    left_high, left_low = split2(left)
    right_high, right_low = split2(right)
    return dot(left_high, right_high, dims) + (
        dot(left_high, right_low, dims) + dot(left_low, right_high, dims)
    )


def mm_exact_left(left, right, dims=NN):
    right_high, right_low = split2(right)
    return dot(left, right_high, dims) + dot(left, right_low, dims)


def mm_exact_right(left, right, dims=NN):
    left_high, left_low = split2(left)
    return dot(left_high, right, dims) + dot(left_low, right, dims)


def away(step, count):
    return min(step, count - step)


def farthest_first(count):
    return sorted(range(1, count), key=lambda step: -away(step, count))


def plane_steps():
    steps = [(up, over) for up in range(NZ) for over in range(NX) if up or over]
    return sorted(steps, key=lambda step: -away(step[0], NZ) - away(step[1], NX))


def local_products(inv, two, one, rhs_t, prod_ref, s_high_ref, s_low_ref, x_ref):
    both = jnp.concatenate((two, one), axis=1)
    both_high, both_low = split2(both)
    inv_high, inv_low = split2(inv)
    solved = dot(inv_high, both_high, NN) + (
        dot(inv_high, both_low, NN) + dot(inv_low, both_high, NN)
    )
    rhs_high, rhs_low = split2(rhs_t)
    x_t = dot(rhs_high, inv_high, NN) + (
        dot(rhs_high, inv_low, NN) + dot(rhs_low, inv_high, NN)
    )
    s_high, s_low = split2(solved)
    grams = dot(both_high, s_high, TN) + (dot(both_high, s_low, TN) + dot(both_low, s_high, TN))
    x_high, x_low = split2(x_t)
    projs = dot(x_high, both_high, NN) + (dot(x_high, both_low, NN) + dot(x_low, both_high, NN))
    shape = (NX, NZ // 2, 8, RANK)
    prod_ref[0, :, :4] = grams[:RANK, :RANK].reshape(shape)
    prod_ref[0, :, 4:] = grams[:RANK, RANK:].reshape(shape)
    prod_ref[1, :, :4] = grams[RANK:, RANK:].reshape(shape)
    prod_ref[1, :2, 4:] = projs[:, :RANK].reshape(2, NZ // 2, 8, RANK)
    prod_ref[1, 2:, 4:] = projs[:, RANK:].reshape(2, NZ // 2, 8, RANK)
    s_high_ref[...] = s_high
    s_low_ref[...] = s_low
    x_ref[...] = x_t


def whole_kernel(
    rhs_hbm, inv_hbm, one_hbm, two_hbm, coarse_hbm, fine_hbm, out_ref,
    s_high_ref, s_low_ref, x_ref, schur_ref, coef_ref,
    rhs_ref, inv_ref, one_ref, two_ref, buf_ref,
    prod_ref, from_core, chip_sum, from_plane, x_sum, by_y,
    work_ref, high_ref, low_ref, coarse_ref, fine_ref, coarse_t, fine_t,
    in_s, core_s, core_r, p_s, p_r, y_s, y_r, gz_s, gz_r, gx_s, gx_r, o_s, o_r,
):
    gx, gy = lax.axis_index("gx"), lax.axis_index("gy")
    y, x_hi = lax.div(gx, 2), lax.rem(gx, 2)
    z, x_lo, core = lax.div(gy, 4), lax.rem(lax.div(gy, 2), 2), lax.rem(gy, 2)
    x = x_hi * 2 + x_lo
    other, solver = 1 - core, lax.div(y, 4)
    sibling = (gx, gy + 1 - 2 * core)

    def plane_peer(up, over):
        z_there, x_there = lax.rem(z + up, NZ), lax.rem(x + over, NX)
        gx_there = y * 2 + lax.div(x_there, 2)
        return z_there, x_there, (gx_there, z_there * 4 + lax.rem(x_there, 2) * 2 + core)

    def z_peer(step):
        there = lax.rem(z + step, NZ)
        return there, (gx, there * 4 + x_lo * 2 + core)

    def x_peer(step):
        there = lax.rem(x + step, NX)
        return there, (y * 2 + lax.div(there, 2), z * 4 + lax.rem(there, 2) * 2 + core)

    loads = [
        pltpu.make_async_copy(source, target, in_s.at[index])
        for index, (source, target) in enumerate(
            ((inv_hbm, inv_ref), (two_hbm, two_ref), (one_hbm, one_ref), (rhs_hbm, rhs_ref),
             (fine_hbm, fine_ref), (coarse_hbm, coarse_ref))
        )
    ]
    for load in loads:
        load.start()

    barrier = pltpu.get_barrier_semaphore()
    peers = [plane_peer(up, over)[2] for up, over in plane_steps()]
    for step in farthest_first(NY):
        there = lax.rem(y + step, NY)
        for which in range(2):
            peers.append((there * 2 + x_hi, z * 4 + x_lo * 2 + which))
    peers += [sibling]
    for peer in peers:
        pl.semaphore_signal(barrier, inc=1, device_id=peer, device_id_type=MESH)

    for load in loads[:4]:
        load.wait()
    local_products(
        inv_ref[...], two_ref[...], one_ref[...], rhs_ref[...],
        prod_ref, s_high_ref, s_low_ref, x_ref,
    )
    pl.semaphore_wait(barrier, len(peers))

    def send(source, target, send_sem, recv_sem, peer):
        copy = pltpu.make_async_remote_copy(
            src_ref=source, dst_ref=target, send_sem=send_sem, recv_sem=recv_sem,
            device_id=peer, device_id_type=MESH,
        )
        copy.start()
        return copy

    first = send(prod_ref.at[other], from_core, core_s, core_r, sibling)
    first.wait()
    for there in range(NX):
        chip_sum[:, there] = prod_ref[core, there] + from_core[there]

    copies = []
    for up, over in plane_steps():
        z_there, x_there, peer = plane_peer(up, over)
        at = up * NX + over - 1
        copies.append(
            send(chip_sum.at[z_there, x_there], from_plane.at[at], p_s.at[at], p_r.at[at], peer)
        )
    for load in loads[4:]:
        load.wait()
    fine_t[...] = fine_ref[core].T
    coarse_t[...] = coarse_ref[0].T
    total = chip_sum[z, x]
    for copy in copies:
        copy.wait()
    for at in range(NZ * NX - 1):
        total = total + from_plane[at]
    x_sum[...] = total

    copies = []
    own = lax.rem(y, 4) * 2 + core
    slot = by_y.at[lax.rem(y, 4), core]
    for step in farthest_first(NY):
        there = lax.rem(y + step, NY)
        peer = (there * 2 + x_hi, z * 4 + x_lo * 2 + solver)
        copies.append(send(x_sum, slot, y_s.at[step - 1], y_r.at[own], peer))

    @pl.when(solver == core)
    def _():
        by_y[lax.rem(y, 4), core] = total

    @pl.when(solver != core)
    def _():
        send(x_sum, slot, y_s.at[7], y_r.at[own], sibling).wait_send()

    for copy in copies:
        copy.wait_send()
    for at in range(8):
        @pl.when(jnp.logical_not(jnp.logical_and(solver == core, own == at)))
        def _():
            pltpu.make_async_remote_copy(
                src_ref=x_sum, dst_ref=by_y.at[at // 2, at % 2], send_sem=y_s.at[0],
                recv_sem=y_r.at[at], device_id=sibling, device_id_type=MESH,
            ).wait_recv()

    for half in range(2):
        for slab in range(2):
            buf_ref[x, z, half, slab] = by_y[2 * slab, half] + by_y[2 * slab + 1, half]

    copies = []
    place = buf_ref.at[x, z]
    for step in farthest_first(NZ):
        _, peer = z_peer(step)
        copies.append(send(place, place, gz_s.at[step - 1], gz_r.at[step - 1], peer))
    for copy in copies:
        copy.wait()

    waves = []
    for wave, (first_z, count_z, half) in enumerate(((0, 4, 0), (4, 4, 0), (0, NZ, 1))):
        place = buf_ref.at[x, pl.ds(first_z, count_z), half]
        copies = []
        for step in farthest_first(NX):
            _, peer = x_peer(step)
            at = wave * 3 + step - 1
            copies.append(send(place, place, gx_s.at[at], gx_r.at[at], peer))
        waves.append(copies)
    for copy in waves[0]:
        copy.wait()

    factor, factor_t = fine_ref[core], fine_t[...]
    cap = capacitance(factor, factor_t, [part(buf_ref, 0, 0), part(buf_ref, 0, 1)])
    eye = identity()
    work_ref[0] = cap[:RANK, :RANK] + eye
    invert_in_place(work_ref, high_ref, low_ref, 1)
    for copy in waves[1] + waves[2]:
        copy.wait()
    mixed = jnp.concatenate((part(buf_ref, 1, 0), part(buf_ref, 1, 1)), axis=0)
    coarse_term = mm_exact_left(factor_t, mixed)
    rights = [part(buf_ref, 3, slab) for slab in range(2)]
    right = jnp.concatenate([rights[slab][:64].T for slab in range(2)], axis=0)
    term = jnp.concatenate((coarse_term, mm_exact_left(factor_t, right)), axis=1)
    wide, first, rest = eliminate(cap, term, work_ref)
    inner = mm(term[:RANK, :RANK], first, TN)
    rest_t = rest[:, :RANK].T
    invert_in_place(work_ref, high_ref, low_ref, 1)
    low = mm(work_ref[0], rest)
    inner = inner + mm(rest_t, low)
    schur_ref[core, :, :RANK] = part(buf_ref, 2, 0) + part(buf_ref, 2, 1) - inner[:, :RANK]
    schur_ref[core, :, RANK:] = (rights[0][64:] + rights[1][64:]).T - inner[:, RANK:]
    schur_swap = send(schur_ref.at[core], schur_ref.at[core], o_s.at[0], o_r.at[0], sibling)
    top = first - mm(wide, low)
    coef_ref[core] = mm_exact_left(factor, jnp.concatenate((top, low), axis=0))
    coef_swap = send(coef_ref.at[core], coef_ref.at[core], o_s.at[1], o_r.at[1], sibling)
    schur_swap.wait()

    block = lax.div(gx, 4)
    my_pair, my_half = lax.div(block, 2), lax.rem(block, 2)
    factor = coarse_ref[0]
    factor_t = coarse_t[...]
    cap = capacitance(factor, factor_t, [schur_ref[0, :, :RANK], schur_ref[1, :, :RANK]])
    term = mm_exact_left(
        factor_t, jnp.concatenate((schur_ref[0, :, RANK:], schur_ref[1, :, RANK:]), axis=0)
    )
    work_ref[0] = cap[:RANK, :RANK] + identity()
    invert_in_place(work_ref, high_ref, low_ref, 1)
    wide, first, rest = eliminate(cap, term, work_ref)
    my_factor = coarse_ref[0, pl.ds(pl.multiple_of(my_pair * RANK, RANK), RANK), :]
    fixed = mm_exact_left(my_factor[:, :RANK], first)
    spare = my_factor[:, RANK:].astype(F32) - mm_exact_left(my_factor[:, :RANK], wide)
    invert_in_place(work_ref, high_ref, low_ref, 1)
    low = mm(work_ref[0], rest)
    m1 = fixed + mm(spare, low)
    coef_swap.wait()
    own = coef_ref[my_pair, pl.ds(pl.multiple_of(my_half * RANK, RANK), RANK), :]
    m2 = own[:, RANK:] - mm(own[:, :RANK], m1)
    weights = jnp.concatenate((m2, m1), axis=0).T
    w_high, w_low = split2(weights)
    s_high = s_high_ref[...]
    out_ref[...] = x_ref[...] - (
        dot(w_high, s_high, NT) + (dot(w_high, s_low_ref[...], NT) + dot(w_low, s_high, NT))
    )


def row_of(tile, index):
    return jnp.broadcast_to(tile[index : index + 1, :], tile.shape)


def spread(tile, pick):
    column = jnp.sum(jnp.where(pick, tile, 0.0), axis=1, keepdims=True)
    return jnp.broadcast_to(column, tile.shape)


def combine(weights, solved):
    sums = [jnp.zeros((8, RANK), F32)] * 4
    for j in range(16):
        sums[j % 4] = sums[j % 4] + weights[j] * row_of(solved[j // 8], j % 8)
    return (sums[0] + sums[1]) + (sums[2] + sums[3])


def panel_solve(tiles, cols, rows):
    scale = [jnp.ones((8, RANK), F32)] * 2
    cols = [list(pair) for pair in cols]
    for k in range(16):
        at, sub = k // 8, k % 8
        pivot = row_of(cols[k][at], sub)
        guess = pl.reciprocal(pivot, approx=True)
        refine = 2.0 - pivot * guess
        inverse = guess * refine
        here = rows == sub
        scale[at] = jnp.where(here, inverse, scale[at])
        raw = list(cols[k])
        raw[at] = jnp.where(here, 0.0, raw[at])
        factors = [value * inverse for value in raw]
        for j in range(k + 1, 16):
            across = row_of(cols[j][at], sub)
            if j == k + 1:
                cols[j] = [cols[j][t] - (raw[t] * across * guess) * refine for t in range(2)]
            else:
                cols[j] = [cols[j][t] - factors[t] * across for t in range(2)]
        across = row_of(tiles[at], sub)
        tiles = [tiles[t] - factors[t] * across for t in range(2)]
    return [tiles[t] * scale[t] for t in range(2)]


def invert_in_place(work_ref, high_ref, low_ref, count):
    rows = lax.broadcasted_iota(jnp.int32, (8, RANK), 0)
    lanes = lax.broadcasted_iota(jnp.int32, (8, RANK), 1)
    tile_count = RANK // 8

    def apply_last(which, base_before, place, before):
        last = jnp.logical_and(lanes >= base_before, lanes < base_before + 16)
        whole = work_ref[which]
        left_high, left_low = split2(whole)
        high, low = high_ref[which], low_ref[which]
        update = dot(left_high, high, NN) + (dot(left_high, low, NN) + dot(left_low, high, NN))
        for tile in range(tile_count):
            at = slice(tile * 8, tile * 8 + 8)
            work_ref[which, at, :] = jnp.where(last, 0.0, whole[at]) - update[at]
        work_ref[which, place, :] = jnp.concatenate(before, axis=0)

    def step(panel, carry):
        base = panel * 16
        inside = jnp.logical_and(lanes >= base, lanes < base + 16)
        earlier = jnp.logical_and(lanes >= base - 16, lanes < base)
        picks = [lanes == base + j for j in range(16)]
        last_picks = [lanes == base - 16 + j for j in range(16)]
        following = lax.rem(base + 32, RANK)
        gone = pl.ds(pl.multiple_of(lax.rem(base + RANK - 16, RANK), 16), 16)
        after = []
        for which in range(count):
            current, coming, before = carry[which]
            old = [[spread(tile, pick) for pick in last_picks] for tile in coming]
            coming = [
                jnp.where(earlier, 0.0, coming[t]) - combine(old[t], before) for t in range(2)
            ]
            weights = [[spread(tile, pick) for pick in picks] for tile in coming]
            cols = [
                [spread(current[t], picks[j]) for t in range(2)]
                for j in range(16)
            ]
            tiles = [
                jnp.where(inside, (lanes - base == rows + 8 * t).astype(F32), current[t])
                for t in range(2)
            ]
            apply_last(which, base - 16, gone, before)
            solved = panel_solve(tiles, cols, rows)
            joined = jnp.concatenate(solved, axis=0)
            high, low = split2(joined)
            high_ref[which, gone, :] = jnp.zeros((16, RANK), BF16)
            low_ref[which, gone, :] = jnp.zeros((16, RANK), BF16)
            at = pl.ds(pl.multiple_of(base, 16), 16)
            high_ref[which, at, :] = high
            low_ref[which, at, :] = low
            upcoming = [
                jnp.where(inside, 0.0, coming[t]) - combine(weights[t], solved) for t in range(2)
            ]
            stale = [
                work_ref[which, pl.ds(pl.multiple_of(following + 8 * t, 8), 8), :] for t in range(2)
            ]
            after.append((tuple(upcoming), tuple(stale), tuple(solved)))
        return tuple(after)

    start = []
    for which in range(count):
        high_ref[which] = jnp.zeros((RANK, RANK), BF16)
        low_ref[which] = jnp.zeros((RANK, RANK), BF16)
        first = (work_ref[which, :8, :], work_ref[which, 8:16, :])
        end = (work_ref[which, 112:120, :], work_ref[which, 120:128, :])
        second = (work_ref[which, 16:24, :], work_ref[which, 24:32, :])
        start.append((first, second, end))
    done = lax.fori_loop(0, RANK // 16, step, tuple(start))
    for which in range(count):
        apply_last(which, RANK - 16, slice(RANK - 16, RANK), done[which][2])


def part(buf_ref, index, slab):
    start = (index % 2) * 4
    return buf_ref[:, start : start + 4, index // 2, slab].reshape(RANK, RANK)


def capacitance(factor, factor_t, grams):
    top = mm_exact_right(grams[0], factor[:RANK])
    low = mm_exact_right(grams[1], factor[RANK:])
    return mm_exact_left(factor_t, jnp.concatenate((top, low), axis=0))


def identity():
    down = lax.broadcasted_iota(jnp.int32, (RANK, RANK), 0)
    return (down == lax.broadcasted_iota(jnp.int32, (RANK, RANK), 1)).astype(F32)


def eliminate(cap, term, work_ref):
    inverse = work_ref[0]
    wide = mm(inverse, cap[:RANK, RANK:])
    cross = cap[RANK:, :RANK]
    work_ref[0] = cap[RANK:, RANK:] + identity() - mm(cross, wide)
    first = mm(inverse, term[:RANK])
    rest = term[RANK:] - mm(cross, first)
    return wide, first, rest


def vmem():
    return pl.BlockSpec(memory_space=pltpu.VMEM)


def shape(*dims, kind=F32):
    return jax.ShapeDtypeStruct(dims, kind)


def inverse_scratch():
    return [
        pltpu.VMEM((1, RANK, RANK), F32),
        pltpu.VMEM((1, RANK, RANK), BF16),
        pltpu.VMEM((1, RANK, RANK), BF16),
    ]


def body(right_side, leaf_inverse, basis_one, basis_two, factor_one, factor_two):
    rows = leaf_inverse.shape[0]
    dma = pltpu.SemaphoreType.DMA
    plane = NZ * NX - 1
    hbm = pl.BlockSpec(memory_space=pltpu.HBM)
    return pl.pallas_call(
        whole_kernel,
        out_shape=shape(64, rows),
        in_specs=[hbm] * 6,
        out_specs=vmem(),
        scratch_shapes=[
            pltpu.VMEM((rows, 2 * RANK), BF16),
            pltpu.VMEM((rows, 2 * RANK), BF16),
            pltpu.VMEM((64, rows), F32),
            pltpu.VMEM((2, RANK, 192), F32),
            pltpu.VMEM((2, 2 * RANK, 192), F32),
            pltpu.VMEM((64, rows), F32),
            pltpu.VMEM((rows, rows), F32),
            pltpu.VMEM((rows, RANK), F32),
            pltpu.VMEM((rows, RANK), F32),
            pltpu.VMEM((NX, NZ, 2, 2, 8, RANK), F32),
            pltpu.VMEM((2, NX, NZ, 8, RANK), F32),
            pltpu.VMEM((NX, NZ, 8, RANK), F32),
            pltpu.VMEM((NZ, NX, 8, RANK), F32),
            pltpu.VMEM((plane, 8, RANK), F32),
            pltpu.VMEM((8, RANK), F32),
            pltpu.VMEM((4, 2, 8, RANK), F32),
        ] + inverse_scratch() + [
            pltpu.VMEM(factor_one.shape, BF16),
            pltpu.VMEM(factor_two.shape, BF16),
            pltpu.VMEM((2 * RANK, 2 * RANK), BF16),
            pltpu.VMEM((2 * RANK, 2 * RANK), BF16),
            dma((6,)), dma, dma, dma((plane,)), dma((plane,)), dma((8,)), dma((8,)),
            dma((7,)), dma((7,)), dma((9,)), dma((9,)), dma((2,)), dma((2,)),
        ],
        compiler_params=pltpu.CompilerParams(
            collective_id=0, has_side_effects=True, vmem_limit_bytes=56_400_000
        ),
    )(right_side.T, leaf_inverse, basis_one, basis_two, factor_one, factor_two).T


def solution(mesh):
    split = P(("gx", "gy"), None)
    return jax.shard_map(
        body, mesh=mesh, in_specs=(split, split, split, split, P(), P()),
        out_specs=split, check_vma=False,
    )
```

```python
import functools

import jax
import jax.numpy as jnp
from jax import lax
from jax.experimental import pallas as pl
from jax.experimental.pallas import tpu as pltpu
from jax.sharding import PartitionSpec as P

MESH = pl.DeviceIdType.MESH
F32 = jnp.float32
BF16 = jnp.bfloat16
RANK = 128
NZ, NX, NY = 8, 4, 8


def split2(value):
    high = value.astype(BF16)
    return high, (value - high.astype(F32)).astype(BF16)


def dot(left, right, dims):
    return lax.dot_general(left, right, (dims, ((), ())), preferred_element_type=F32)


NN = ((1,), (0,))
TN = ((0,), (0,))
NT = ((1,), (1,))


def mm(left, right, dims=NN):
    left_high, left_low = split2(left)
    right_high, right_low = split2(right)
    return dot(left_high, right_high, dims) + (
        dot(left_high, right_low, dims) + dot(left_low, right_high, dims)
    )


def mm_exact_left(left, right, dims=NN):
    right_high, right_low = split2(right)
    return dot(left, right_high, dims) + dot(left, right_low, dims)


def mm_exact_right(left, right, dims=NN):
    left_high, left_low = split2(left)
    return dot(left_high, right, dims) + dot(left_low, right, dims)


def away(step, count):
    return min(step, count - step)


def farthest_first(count):
    return sorted(range(1, count), key=lambda step: -away(step, count))


def plane_steps():
    steps = [(up, over) for up in range(NZ) for over in range(NX) if up or over]
    return sorted(steps, key=lambda step: -away(step[0], NZ) - away(step[1], NX))


def local_products(inv, two, one, rhs_t, prod_ref, s_high_ref, s_low_ref, x_ref):
    both = jnp.concatenate((two, one), axis=1)
    both_high, both_low = split2(both)
    inv_high, inv_low = split2(inv)
    solved = dot(inv_high, both_high, NN) + (
        dot(inv_high, both_low, NN) + dot(inv_low, both_high, NN)
    )
    rhs_high, rhs_low = split2(rhs_t)
    x_t = dot(rhs_high, inv_high, NN) + (
        dot(rhs_high, inv_low, NN) + dot(rhs_low, inv_high, NN)
    )
    s_high, s_low = split2(solved)
    grams = dot(both_high, s_high, TN) + (dot(both_high, s_low, TN) + dot(both_low, s_high, TN))
    x_high, x_low = split2(x_t)
    projs = dot(x_high, both_high, NN) + (dot(x_high, both_low, NN) + dot(x_low, both_high, NN))
    shape = (NX, NZ // 2, 8, RANK)
    prod_ref[0, :, :4] = grams[:RANK, :RANK].reshape(shape)
    prod_ref[0, :, 4:] = grams[:RANK, RANK:].reshape(shape)
    prod_ref[1, :, :4] = grams[RANK:, RANK:].reshape(shape)
    prod_ref[1, :2, 4:] = projs[:, :RANK].reshape(2, NZ // 2, 8, RANK)
    prod_ref[1, 2:, 4:] = projs[:, RANK:].reshape(2, NZ // 2, 8, RANK)
    s_high_ref[...] = s_high
    s_low_ref[...] = s_low
    x_ref[...] = x_t


def whole_kernel(
    rhs_hbm, inv_hbm, one_hbm, two_hbm, coarse_hbm, fine_hbm, out_ref,
    s_high_ref, s_low_ref, x_ref, schur_ref, coef_ref,
    rhs_ref, inv_ref, one_ref, two_ref, buf_ref,
    prod_ref, from_core, chip_sum, from_plane, x_sum, by_y,
    work_ref, high_ref, low_ref, coarse_ref, fine_ref, coarse_t, fine_t, s_high_t, s_low_t,
    in_s, core_s, core_r, p_s, p_r, y_s, y_r, gz_s, gz_r, gx_s, gx_r, o_s, o_r,
):
    gx, gy = lax.axis_index("gx"), lax.axis_index("gy")
    y, x_hi = lax.div(gx, 2), lax.rem(gx, 2)
    z, x_lo, core = lax.div(gy, 4), lax.rem(lax.div(gy, 2), 2), lax.rem(gy, 2)
    x = x_hi * 2 + x_lo
    other, solver = 1 - core, lax.div(y, 4)
    sibling = (gx, gy + 1 - 2 * core)

    def plane_peer(up, over):
        z_there, x_there = lax.rem(z + up, NZ), lax.rem(x + over, NX)
        gx_there = y * 2 + lax.div(x_there, 2)
        return z_there, x_there, (gx_there, z_there * 4 + lax.rem(x_there, 2) * 2 + core)

    def z_peer(step):
        there = lax.rem(z + step, NZ)
        return there, (gx, there * 4 + x_lo * 2 + core)

    def x_peer(step):
        there = lax.rem(x + step, NX)
        return there, (y * 2 + lax.div(there, 2), z * 4 + lax.rem(there, 2) * 2 + core)

    loads = [
        pltpu.make_async_copy(source, target, in_s.at[index])
        for index, (source, target) in enumerate(
            ((inv_hbm, inv_ref), (two_hbm, two_ref), (one_hbm, one_ref), (rhs_hbm, rhs_ref),
             (fine_hbm, fine_ref), (coarse_hbm, coarse_ref))
        )
    ]
    for load in loads:
        load.start()

    barrier = pltpu.get_barrier_semaphore()
    peers = [plane_peer(up, over)[2] for up, over in plane_steps()]
    for step in farthest_first(NY):
        there = lax.rem(y + step, NY)
        for which in range(2):
            peers.append((there * 2 + x_hi, z * 4 + x_lo * 2 + which))
    peers += [sibling]
    for peer in peers:
        pl.semaphore_signal(barrier, inc=1, device_id=peer, device_id_type=MESH)

    for load in loads[:4]:
        load.wait()
    local_products(
        inv_ref[...], two_ref[...], one_ref[...], rhs_ref[...],
        prod_ref, s_high_ref, s_low_ref, x_ref,
    )
    pl.semaphore_wait(barrier, len(peers))

    def send(source, target, send_sem, recv_sem, peer):
        copy = pltpu.make_async_remote_copy(
            src_ref=source, dst_ref=target, send_sem=send_sem, recv_sem=recv_sem,
            device_id=peer, device_id_type=MESH,
        )
        copy.start()
        return copy

    first = send(prod_ref.at[other], from_core, core_s, core_r, sibling)
    first.wait()
    for there in range(NX):
        chip_sum[:, there] = prod_ref[core, there] + from_core[there]

    copies = []
    for up, over in plane_steps():
        z_there, x_there, peer = plane_peer(up, over)
        at = up * NX + over - 1
        copies.append(
            send(chip_sum.at[z_there, x_there], from_plane.at[at], p_s.at[at], p_r.at[at], peer)
        )
    for load in loads[4:]:
        load.wait()
    fine_t[...] = fine_ref[core].T
    s_high_t[...] = s_high_ref[...].T
    s_low_t[...] = s_low_ref[...].T
    coarse_t[...] = coarse_ref[0].T
    total = chip_sum[z, x]
    for copy in copies:
        copy.wait()
    for at in range(NZ * NX - 1):
        total = total + from_plane[at]
    x_sum[...] = total

    copies = []
    own = lax.rem(y, 4) * 2 + core
    slot = by_y.at[lax.rem(y, 4), core]
    for step in farthest_first(NY):
        there = lax.rem(y + step, NY)
        peer = (there * 2 + x_hi, z * 4 + x_lo * 2 + solver)
        copies.append(send(x_sum, slot, y_s.at[step - 1], y_r.at[own], peer))

    @pl.when(solver == core)
    def _():
        by_y[lax.rem(y, 4), core] = total

    @pl.when(solver != core)
    def _():
        send(x_sum, slot, y_s.at[7], y_r.at[own], sibling).wait_send()

    for copy in copies:
        copy.wait_send()
    for at in range(8):
        @pl.when(jnp.logical_not(jnp.logical_and(solver == core, own == at)))
        def _():
            pltpu.make_async_remote_copy(
                src_ref=x_sum, dst_ref=by_y.at[at // 2, at % 2], send_sem=y_s.at[0],
                recv_sem=y_r.at[at], device_id=sibling, device_id_type=MESH,
            ).wait_recv()

    for half in range(2):
        for slab in range(2):
            buf_ref[x, z, half, slab] = by_y[2 * slab, half] + by_y[2 * slab + 1, half]

    over_z = []
    for half in range(2):
        place = buf_ref.at[x, z, half]
        copies = []
        for step in farthest_first(NZ):
            _, peer = z_peer(step)
            at = half * 7 + step - 1
            copies.append(send(place, place, gz_s.at[at], gz_r.at[at], peer))
        over_z.append(copies)

    waves = []
    for wave, (first_z, count_z, half) in enumerate(((0, 4, 0), (4, 4, 0), (0, NZ, 1))):
        if wave != 1:
            for copy in over_z[half]:
                copy.wait()
        place = buf_ref.at[x, pl.ds(first_z, count_z), half]
        copies = []
        for step in farthest_first(NX):
            _, peer = x_peer(step)
            at = wave * 3 + step - 1
            copies.append(send(place, place, gx_s.at[at], gx_r.at[at], peer))
        waves.append(copies)
    for copy in waves[0]:
        copy.wait()

    factor, factor_t = fine_ref[core], fine_t[...]
    cap = capacitance(factor, factor_t, [part(buf_ref, 0, 0), part(buf_ref, 0, 1)])
    eye = identity()
    work_ref[0] = cap[:RANK, :RANK] + eye
    invert_in_place(work_ref, high_ref, low_ref)
    for copy in waves[1] + waves[2]:
        copy.wait()
    mixed = jnp.concatenate((part(buf_ref, 1, 0), part(buf_ref, 1, 1)), axis=0)
    coarse_term = mm_exact_left(factor_t, mixed)
    rights = [part(buf_ref, 3, slab) for slab in range(2)]
    right = jnp.concatenate([rights[slab][:64].T for slab in range(2)], axis=0)
    term = jnp.concatenate((coarse_term, mm_exact_left(factor_t, right)), axis=1)
    wide, first, rest = eliminate(cap, term, work_ref)
    inner = mm(term[:RANK, :RANK], first, TN)
    rest_t = rest[:, :RANK].T
    invert_in_place(work_ref, high_ref, low_ref)
    low = mm(work_ref[0], rest)
    inner = inner + mm(rest_t, low)
    schur_ref[core, :, :RANK] = part(buf_ref, 2, 0) + part(buf_ref, 2, 1) - inner[:, :RANK]
    schur_ref[core, :, RANK:] = (rights[0][64:] + rights[1][64:]).T - inner[:, RANK:]
    schur_swap = send(schur_ref.at[core], schur_ref.at[core], o_s.at[0], o_r.at[0], sibling)
    top = first - mm(wide, low)
    coef_ref[core] = mm_exact_left(factor, jnp.concatenate((top, low), axis=0))
    coef_swap = send(coef_ref.at[core], coef_ref.at[core], o_s.at[1], o_r.at[1], sibling)
    schur_swap.wait()

    block = lax.div(gx, 4)
    my_pair, my_half = lax.div(block, 2), lax.rem(block, 2)
    factor = coarse_ref[0]
    factor_t = coarse_t[...]
    cap = capacitance(factor, factor_t, [schur_ref[0, :, :RANK], schur_ref[1, :, :RANK]])
    term = mm_exact_left(
        factor_t, jnp.concatenate((schur_ref[0, :, RANK:], schur_ref[1, :, RANK:]), axis=0)
    )
    work_ref[0] = cap[:RANK, :RANK] + identity()
    invert_in_place(work_ref, high_ref, low_ref)
    wide, first, rest = eliminate(cap, term, work_ref)
    my_factor = coarse_ref[0, pl.ds(pl.multiple_of(my_pair * RANK, RANK), RANK), :]
    fixed_t = mm_exact_left(my_factor[:, :RANK], first).T
    spare = my_factor[:, RANK:].astype(F32) - mm_exact_left(my_factor[:, :RANK], wide)
    spare_t, rest_t = spare.T, rest.T
    coef_swap.wait()
    own = coef_ref[my_pair, pl.ds(pl.multiple_of(my_half * RANK, RANK), RANK), :]
    own_s_t, own_x_t = own[:, :RANK].T, own[:, RANK:].T
    invert_in_place(work_ref, high_ref, low_ref)
    m1_t = fixed_t + mm(mm(rest_t, work_ref[0]), spare_t)
    m2_t = own_x_t - mm(m1_t, own_s_t)
    w_high, w_low = split2(jnp.concatenate((m2_t, m1_t), axis=1))
    s_high = s_high_t[...]
    out_ref[...] = x_ref[...] - (
        dot(w_high, s_high, NN) + (dot(w_high, s_low_t[...], NN) + dot(w_low, s_high, NN))
    )


def row_of(tile, index):
    return jnp.broadcast_to(tile[index : index + 1, :], tile.shape)


def spread(tile, pick):
    column = jnp.sum(jnp.where(pick, tile, 0.0), axis=1, keepdims=True)
    return jnp.broadcast_to(column, tile.shape)


def combine(weights, solved):
    sums = [jnp.zeros((8, RANK), F32)] * 4
    for j in range(16):
        sums[j % 4] = sums[j % 4] + weights[j] * row_of(solved[j // 8], j % 8)
    return (sums[0] + sums[1]) + (sums[2] + sums[3])


def panel_solve(tiles, cols, rows):
    scale = [jnp.ones((8, RANK), F32)] * 2
    cols = [list(pair) for pair in cols]
    for k in range(16):
        at, sub = k // 8, k % 8
        pivot = row_of(cols[k][at], sub)
        guess = pl.reciprocal(pivot, approx=True)
        refine = 2.0 - pivot * guess
        inverse = guess * refine
        here = rows == sub
        scale[at] = jnp.where(here, inverse, scale[at])
        raw = list(cols[k])
        raw[at] = jnp.where(here, 0.0, raw[at])
        factors = [value * inverse for value in raw]
        for j in range(k + 1, 16):
            across = row_of(cols[j][at], sub)
            if j == k + 1:
                cols[j] = [cols[j][t] - (raw[t] * across * guess) * refine for t in range(2)]
            else:
                cols[j] = [cols[j][t] - factors[t] * across for t in range(2)]
        across = row_of(tiles[at], sub)
        tiles = [tiles[t] - factors[t] * across for t in range(2)]
    return [tiles[t] * scale[t] for t in range(2)]


def invert_in_place(work_ref, high_ref, low_ref, count=1):
    rows = lax.broadcasted_iota(jnp.int32, (8, RANK), 0)
    lanes = lax.broadcasted_iota(jnp.int32, (8, RANK), 1)
    ends = RANK - 16

    def apply_last(base_before, place, before):
        last = jnp.logical_and(lanes >= base_before, lanes < base_before + 16)
        whole = work_ref[0]
        left_high, left_low = split2(whole)
        high, low = high_ref[0], low_ref[0]
        update = dot(left_high, high, NN) + (dot(left_high, low, NN) + dot(left_low, high, NN))
        for tile in range(RANK // 8):
            at = slice(tile * 8, tile * 8 + 8)
            work_ref[0, at, :] = jnp.where(last, 0.0, whole[at]) - update[at]
        work_ref[0, place, :] = jnp.concatenate(before, axis=0)

    def reduce_panel(base, current):
        inside = jnp.logical_and(lanes >= base, lanes < base + 16)
        picks = [lanes == base + j for j in range(16)]
        cols = [[spread(current[t], pick) for t in range(2)] for pick in picks]
        tiles = [
            jnp.where(inside, (lanes - base == rows + 8 * t).astype(F32), current[t])
            for t in range(2)
        ]
        return inside, picks, tiles, cols

    def keep(solved, gone, at):
        high, low = split2(jnp.concatenate(solved, axis=0))
        high_ref[0, gone, :] = jnp.zeros((16, RANK), BF16)
        low_ref[0, gone, :] = jnp.zeros((16, RANK), BF16)
        high_ref[0, at, :] = high
        low_ref[0, at, :] = low

    def step(panel, carry):
        current, coming, before = carry
        base = panel * 16
        gone = pl.ds(pl.multiple_of(lax.rem(base + ends, RANK), 16), 16)
        following = lax.rem(base + 32, RANK)
        inside, picks, tiles, cols = reduce_panel(base, current)
        earlier = jnp.logical_and(lanes >= base - 16, lanes < base)
        old = [[spread(tile, lanes == base - 16 + j) for j in range(16)] for tile in coming]
        coming = [jnp.where(earlier, 0.0, coming[t]) - combine(old[t], before) for t in range(2)]
        weights = [[spread(tile, pick) for pick in picks] for tile in coming]
        apply_last(base - 16, gone, before)
        solved = panel_solve(tiles, cols, rows)
        keep(solved, gone, pl.ds(pl.multiple_of(base, 16), 16))
        upcoming = tuple(
            jnp.where(inside, 0.0, coming[t]) - combine(weights[t], solved) for t in range(2)
        )
        stale = tuple(
            work_ref[0, pl.ds(pl.multiple_of(following + 8 * t, 8), 8), :] for t in range(2)
        )
        return upcoming, stale, tuple(solved)

    high_ref[0] = jnp.zeros((RANK, RANK), BF16)
    low_ref[0] = jnp.zeros((RANK, RANK), BF16)
    tile_at = lambda start: work_ref[0, start : start + 8, :]
    start = ((tile_at(0), tile_at(8)), (tile_at(16), tile_at(24)), (tile_at(112), tile_at(120)))
    current, _, before = lax.fori_loop(0, RANK // 16 - 1, step, start)
    _, _, tiles, cols = reduce_panel(ends, current)
    apply_last(ends - 16, slice(ends - 16, ends), before)
    solved = panel_solve(tiles, cols, rows)
    keep(solved, slice(ends - 16, ends), slice(ends, RANK))
    apply_last(ends, slice(ends, RANK), solved)


def part(buf_ref, index, slab):
    start = (index % 2) * 4
    return buf_ref[:, start : start + 4, index // 2, slab].reshape(RANK, RANK)


def capacitance(factor, factor_t, grams):
    top = mm_exact_right(grams[0], factor[:RANK])
    low = mm_exact_right(grams[1], factor[RANK:])
    return mm_exact_left(factor_t, jnp.concatenate((top, low), axis=0))


def identity():
    down = lax.broadcasted_iota(jnp.int32, (RANK, RANK), 0)
    return (down == lax.broadcasted_iota(jnp.int32, (RANK, RANK), 1)).astype(F32)


def eliminate(cap, term, work_ref):
    inverse = work_ref[0]
    wide = mm(inverse, cap[:RANK, RANK:])
    cross = cap[RANK:, :RANK]
    work_ref[0] = cap[RANK:, RANK:] + identity() - mm(cross, wide)
    first = mm(inverse, term[:RANK])
    rest = term[RANK:] - mm(cross, first)
    return wide, first, rest


def vmem():
    return pl.BlockSpec(memory_space=pltpu.VMEM)


def shape(*dims, kind=F32):
    return jax.ShapeDtypeStruct(dims, kind)


def inverse_scratch():
    return [
        pltpu.VMEM((1, RANK, RANK), F32),
        pltpu.VMEM((1, RANK, RANK), BF16),
        pltpu.VMEM((1, RANK, RANK), BF16),
    ]


def body(right_side, leaf_inverse, basis_one, basis_two, factor_one, factor_two):
    rows = leaf_inverse.shape[0]
    dma = pltpu.SemaphoreType.DMA
    plane = NZ * NX - 1
    hbm = pl.BlockSpec(memory_space=pltpu.HBM)
    return pl.pallas_call(
        whole_kernel,
        out_shape=shape(64, rows),
        in_specs=[hbm] * 6,
        out_specs=vmem(),
        scratch_shapes=[
            pltpu.VMEM((rows, 2 * RANK), BF16),
            pltpu.VMEM((rows, 2 * RANK), BF16),
            pltpu.VMEM((64, rows), F32),
            pltpu.VMEM((2, RANK, 192), F32),
            pltpu.VMEM((2, 2 * RANK, 192), F32),
            pltpu.VMEM((64, rows), F32),
            pltpu.VMEM((rows, rows), F32),
            pltpu.VMEM((rows, RANK), F32),
            pltpu.VMEM((rows, RANK), F32),
            pltpu.VMEM((NX, NZ, 2, 2, 8, RANK), F32),
            pltpu.VMEM((2, NX, NZ, 8, RANK), F32),
            pltpu.VMEM((NX, NZ, 8, RANK), F32),
            pltpu.VMEM((NZ, NX, 8, RANK), F32),
            pltpu.VMEM((plane, 8, RANK), F32),
            pltpu.VMEM((8, RANK), F32),
            pltpu.VMEM((4, 2, 8, RANK), F32),
        ] + inverse_scratch() + [
            pltpu.VMEM(factor_one.shape, BF16),
            pltpu.VMEM(factor_two.shape, BF16),
            pltpu.VMEM((2 * RANK, 2 * RANK), BF16),
            pltpu.VMEM((2 * RANK, 2 * RANK), BF16),
            pltpu.VMEM((2 * RANK, rows), BF16),
            pltpu.VMEM((2 * RANK, rows), BF16),
            dma((6,)), dma, dma, dma((plane,)), dma((plane,)), dma((8,)), dma((8,)),
            dma((14,)), dma((14,)), dma((9,)), dma((9,)), dma((2,)), dma((2,)),
        ],
        compiler_params=pltpu.CompilerParams(
            collective_id=0, has_side_effects=True, vmem_limit_bytes=56_400_000
        ),
    )(right_side.T, leaf_inverse, basis_one, basis_two, factor_one, factor_two).T


def solution(mesh):
    split = P(("gx", "gy"), None)
    return jax.shard_map(
        body, mesh=mesh, in_specs=(split, split, split, split, P(), P()),
        out_specs=split, check_vma=False,
    )
```

```python
import functools

import jax
import jax.numpy as jnp
from jax import lax
from jax.experimental import pallas as pl
from jax.experimental.pallas import tpu as pltpu
from jax.sharding import PartitionSpec as P

MESH = pl.DeviceIdType.MESH
F32 = jnp.float32
BF16 = jnp.bfloat16
RANK = 128
NZ, NX, NY = 8, 4, 8


def split2(value):
    high = value.astype(BF16)
    return high, (value - high.astype(F32)).astype(BF16)


def dot(left, right, dims):
    return lax.dot_general(left, right, (dims, ((), ())), preferred_element_type=F32)


NN = ((1,), (0,))
TN = ((0,), (0,))
NT = ((1,), (1,))


def mm(left, right, dims=NN):
    left_high, left_low = split2(left)
    right_high, right_low = split2(right)
    return dot(left_high, right_high, dims) + (
        dot(left_high, right_low, dims) + dot(left_low, right_high, dims)
    )


def mm_exact_left(left, right, dims=NN):
    right_high, right_low = split2(right)
    return dot(left, right_high, dims) + dot(left, right_low, dims)


def mm_exact_right(left, right, dims=NN):
    left_high, left_low = split2(left)
    return dot(left_high, right, dims) + dot(left_low, right, dims)


def away(step, count):
    return min(step, count - step)


def farthest_first(count):
    return sorted(range(1, count), key=lambda step: -away(step, count))


def plane_steps():
    steps = [(up, over) for up in range(NZ) for over in range(NX) if up or over]
    return sorted(steps, key=lambda step: -away(step[0], NZ) - away(step[1], NX))


def local_products(
    inv_ref, two_ref, one_ref, rhs_ref, loads, prod_ref, s_high_ref, s_low_ref, x_ref
):
    for load in loads[1:]:
        load.wait()
    both_high, both_low = split2(jnp.concatenate((two_ref[...], one_ref[...]), axis=1))
    rhs_high, rhs_low = split2(rhs_ref[...])
    loads[0].wait()
    inv_high, inv_low = split2(inv_ref[...])
    solved = dot(inv_high, both_high, NN) + (
        dot(inv_high, both_low, NN) + dot(inv_low, both_high, NN)
    )
    x_t = dot(rhs_high, inv_high, NN) + (
        dot(rhs_high, inv_low, NN) + dot(rhs_low, inv_high, NN)
    )
    s_high, s_low = split2(solved)
    grams = dot(both_high, s_high, TN) + (dot(both_high, s_low, TN) + dot(both_low, s_high, TN))
    x_high, x_low = split2(x_t)
    projs = dot(x_high, both_high, NN) + (dot(x_high, both_low, NN) + dot(x_low, both_high, NN))
    shape = (NX, NZ // 2, 8, RANK)
    prod_ref[0, :, :4] = grams[:RANK, :RANK].reshape(shape)
    prod_ref[0, :, 4:] = grams[:RANK, RANK:].reshape(shape)
    prod_ref[1, :, :4] = grams[RANK:, RANK:].reshape(shape)
    prod_ref[1, :2, 4:] = projs[:, :RANK].reshape(2, NZ // 2, 8, RANK)
    prod_ref[1, 2:, 4:] = projs[:, RANK:].reshape(2, NZ // 2, 8, RANK)
    s_high_ref[...] = s_high
    s_low_ref[...] = s_low
    x_ref[...] = x_t


def whole_kernel(
    rhs_hbm, inv_hbm, one_hbm, two_hbm, coarse_hbm, fine_hbm, out_ref,
    s_high_ref, s_low_ref, x_ref, schur_ref, coef_ref,
    rhs_ref, inv_ref, one_ref, two_ref, buf_ref,
    prod_ref, from_core, chip_sum, from_plane, x_sum, by_y,
    work_ref, high_ref, low_ref, coarse_ref, fine_ref, coarse_t, fine_t, s_high_t, s_low_t,
    in_s, core_s, core_r, p_s, p_r, y_s, y_r, gz_s, gz_r, gx_s, gx_r, o_s, o_r,
):
    gx, gy = lax.axis_index("gx"), lax.axis_index("gy")
    y, x_hi = lax.div(gx, 2), lax.rem(gx, 2)
    z, x_lo, core = lax.div(gy, 4), lax.rem(lax.div(gy, 2), 2), lax.rem(gy, 2)
    x = x_hi * 2 + x_lo
    other, solver = 1 - core, lax.div(y, 4)
    sibling = (gx, gy + 1 - 2 * core)

    def plane_peer(up, over):
        z_there, x_there = lax.rem(z + up, NZ), lax.rem(x + over, NX)
        gx_there = y * 2 + lax.div(x_there, 2)
        return z_there, x_there, (gx_there, z_there * 4 + lax.rem(x_there, 2) * 2 + core)

    def z_peer(step):
        there = lax.rem(z + step, NZ)
        return there, (gx, there * 4 + x_lo * 2 + core)

    def x_peer(step):
        there = lax.rem(x + step, NX)
        return there, (y * 2 + lax.div(there, 2), z * 4 + lax.rem(there, 2) * 2 + core)

    loads = [
        pltpu.make_async_copy(source, target, in_s.at[index])
        for index, (source, target) in enumerate(
            ((inv_hbm, inv_ref), (two_hbm, two_ref), (one_hbm, one_ref), (rhs_hbm, rhs_ref),
             (fine_hbm, fine_ref), (coarse_hbm, coarse_ref))
        )
    ]
    for load in loads:
        load.start()

    barrier = pltpu.get_barrier_semaphore()
    peers = [plane_peer(up, over)[2] for up, over in plane_steps()]
    for step in farthest_first(NY):
        there = lax.rem(y + step, NY)
        for which in range(2):
            peers.append((there * 2 + x_hi, z * 4 + x_lo * 2 + which))
    peers += [sibling]
    for peer in peers:
        pl.semaphore_signal(barrier, inc=1, device_id=peer, device_id_type=MESH)

    local_products(
        inv_ref, two_ref, one_ref, rhs_ref, loads[:4], prod_ref, s_high_ref, s_low_ref, x_ref
    )
    pl.semaphore_wait(barrier, len(peers))

    def send(source, target, send_sem, recv_sem, peer):
        copy = pltpu.make_async_remote_copy(
            src_ref=source, dst_ref=target, send_sem=send_sem, recv_sem=recv_sem,
            device_id=peer, device_id_type=MESH,
        )
        copy.start()
        return copy

    first = send(prod_ref.at[other], from_core, core_s, core_r, sibling)
    first.wait()
    for there in range(NX):
        chip_sum[:, there] = prod_ref[core, there] + from_core[there]

    copies = []
    for up, over in plane_steps():
        z_there, x_there, peer = plane_peer(up, over)
        at = up * NX + over - 1
        copies.append(
            send(chip_sum.at[z_there, x_there], from_plane.at[at], p_s.at[at], p_r.at[at], peer)
        )
    for load in loads[4:]:
        load.wait()
    fine_t[...] = fine_ref[core].T
    s_high_t[...] = s_high_ref[...].T
    s_low_t[...] = s_low_ref[...].T
    coarse_t[...] = coarse_ref[0].T
    total = chip_sum[z, x]
    for copy in copies:
        copy.wait()
    for at in range(NZ * NX - 1):
        total = total + from_plane[at]
    x_sum[...] = total

    copies = []
    own = lax.rem(y, 4) * 2 + core
    slot = by_y.at[lax.rem(y, 4), core]
    for step in farthest_first(NY):
        there = lax.rem(y + step, NY)
        peer = (there * 2 + x_hi, z * 4 + x_lo * 2 + solver)
        copies.append(send(x_sum, slot, y_s.at[step - 1], y_r.at[own], peer))

    @pl.when(solver == core)
    def _():
        by_y[lax.rem(y, 4), core] = total

    @pl.when(solver != core)
    def _():
        send(x_sum, slot, y_s.at[7], y_r.at[own], sibling).wait_send()

    for copy in copies:
        copy.wait_send()
    for at in range(8):
        @pl.when(jnp.logical_not(jnp.logical_and(solver == core, own == at)))
        def _():
            pltpu.make_async_remote_copy(
                src_ref=x_sum, dst_ref=by_y.at[at // 2, at % 2], send_sem=y_s.at[0],
                recv_sem=y_r.at[at], device_id=sibling, device_id_type=MESH,
            ).wait_recv()

    for half in range(2):
        for slab in range(2):
            buf_ref[x, z, half, slab] = by_y[2 * slab, half] + by_y[2 * slab + 1, half]

    over_z = []
    for half in range(2):
        place = buf_ref.at[x, z, half]
        copies = []
        for step in farthest_first(NZ):
            _, peer = z_peer(step)
            at = half * 7 + step - 1
            copies.append(send(place, place, gz_s.at[at], gz_r.at[at], peer))
        over_z.append(copies)

    waves = []
    for wave, (first_z, count_z, half) in enumerate(((0, 4, 0), (4, 4, 0), (0, NZ, 1))):
        if wave != 1:
            for copy in over_z[half]:
                copy.wait()
        place = buf_ref.at[x, pl.ds(first_z, count_z), half]
        copies = []
        for step in farthest_first(NX):
            _, peer = x_peer(step)
            at = wave * 3 + step - 1
            copies.append(send(place, place, gx_s.at[at], gx_r.at[at], peer))
        waves.append(copies)
    for copy in waves[0]:
        copy.wait()

    factor, factor_t = fine_ref[core], fine_t[...]
    cap = capacitance(factor, factor_t, [part(buf_ref, 0, 0), part(buf_ref, 0, 1)])
    eye = identity()
    work_ref[0] = cap[:RANK, :RANK] + eye
    invert_in_place(work_ref, high_ref, low_ref)
    for copy in waves[1] + waves[2]:
        copy.wait()
    mixed = jnp.concatenate((part(buf_ref, 1, 0), part(buf_ref, 1, 1)), axis=0)
    coarse_term = mm_exact_left(factor_t, mixed)
    rights = [part(buf_ref, 3, slab) for slab in range(2)]
    right = jnp.concatenate([rights[slab][:64].T for slab in range(2)], axis=0)
    term = jnp.concatenate((coarse_term, mm_exact_left(factor_t, right)), axis=1)
    wide, first, rest = eliminate(cap, term, work_ref)
    inner = mm(term[:RANK, :RANK], first, TN)
    rest_t = rest[:, :RANK].T
    invert_in_place(work_ref, high_ref, low_ref)
    low = mm(work_ref[0], rest)
    inner = inner + mm(rest_t, low)
    schur_ref[core, :, :RANK] = part(buf_ref, 2, 0) + part(buf_ref, 2, 1) - inner[:, :RANK]
    schur_ref[core, :, RANK:] = (rights[0][64:] + rights[1][64:]).T - inner[:, RANK:]
    schur_swap = send(schur_ref.at[core], schur_ref.at[core], o_s.at[0], o_r.at[0], sibling)
    top = first - mm(wide, low)
    coef_ref[core] = mm_exact_left(factor, jnp.concatenate((top, low), axis=0))
    coef_swap = send(coef_ref.at[core], coef_ref.at[core], o_s.at[1], o_r.at[1], sibling)
    schur_swap.wait()

    block = lax.div(gx, 4)
    my_pair, my_half = lax.div(block, 2), lax.rem(block, 2)
    factor = coarse_ref[0]
    factor_t = coarse_t[...]
    cap = capacitance(factor, factor_t, [schur_ref[0, :, :RANK], schur_ref[1, :, :RANK]])
    term = mm_exact_left(
        factor_t, jnp.concatenate((schur_ref[0, :, RANK:], schur_ref[1, :, RANK:]), axis=0)
    )
    work_ref[0] = cap[:RANK, :RANK] + identity()
    invert_in_place(work_ref, high_ref, low_ref)
    wide, first, rest = eliminate(cap, term, work_ref)
    my_factor = coarse_ref[0, pl.ds(pl.multiple_of(my_pair * RANK, RANK), RANK), :]
    fixed_t = mm_exact_left(my_factor[:, :RANK], first).T
    spare = my_factor[:, RANK:].astype(F32) - mm_exact_left(my_factor[:, :RANK], wide)
    spare_t, rest_t = spare.T, rest.T
    coef_swap.wait()
    own = coef_ref[my_pair, pl.ds(pl.multiple_of(my_half * RANK, RANK), RANK), :]
    own_s_t, own_x_t = own[:, :RANK].T, own[:, RANK:].T
    invert_in_place(work_ref, high_ref, low_ref)
    m1_t = fixed_t + mm(mm(rest_t, work_ref[0]), spare_t)
    m2_t = own_x_t - mm(m1_t, own_s_t)
    w_high, w_low = split2(jnp.concatenate((m2_t, m1_t), axis=1))
    s_high = s_high_t[...]
    out_ref[...] = x_ref[...] - (
        dot(w_high, s_high, NN) + (dot(w_high, s_low_t[...], NN) + dot(w_low, s_high, NN))
    )


def row_of(tile, index):
    return jnp.broadcast_to(tile[index : index + 1, :], tile.shape)


def spread(tile, pick):
    column = jnp.sum(jnp.where(pick, tile, 0.0), axis=1, keepdims=True)
    return jnp.broadcast_to(column, tile.shape)


def combine(weights, solved):
    sums = [jnp.zeros((8, RANK), F32)] * 4
    for j in range(16):
        sums[j % 4] = sums[j % 4] + weights[j] * row_of(solved[j // 8], j % 8)
    return (sums[0] + sums[1]) + (sums[2] + sums[3])


def panel_solve(tiles, cols, rows):
    scale = [jnp.ones((8, RANK), F32)] * 2
    cols = [list(pair) for pair in cols]
    for k in range(16):
        at, sub = k // 8, k % 8
        pivot = row_of(cols[k][at], sub)
        guess = pl.reciprocal(pivot, approx=True)
        refine = 2.0 - pivot * guess
        inverse = guess * refine
        here = rows == sub
        scale[at] = jnp.where(here, inverse, scale[at])
        raw = list(cols[k])
        raw[at] = jnp.where(here, 0.0, raw[at])
        factors = [value * inverse for value in raw]
        for j in range(k + 1, 16):
            across = row_of(cols[j][at], sub)
            if j == k + 1:
                cols[j] = [cols[j][t] - raw[t] * guess * across * refine for t in range(2)]
            else:
                cols[j] = [cols[j][t] - factors[t] * across for t in range(2)]
        across = row_of(tiles[at], sub)
        tiles = [tiles[t] - factors[t] * across for t in range(2)]
    return [tiles[t] * scale[t] for t in range(2)]


def invert_in_place(work_ref, high_ref, low_ref, count=1):
    rows = lax.broadcasted_iota(jnp.int32, (8, RANK), 0)
    lanes = lax.broadcasted_iota(jnp.int32, (8, RANK), 1)
    ends = RANK - 16

    def apply_last(base_before, place, before):
        last = jnp.logical_and(lanes >= base_before, lanes < base_before + 16)
        whole = work_ref[0]
        left_high, left_low = split2(whole)
        high, low = high_ref[0], low_ref[0]
        update = dot(left_high, high, NN) + (dot(left_high, low, NN) + dot(left_low, high, NN))
        for tile in range(RANK // 8):
            at = slice(tile * 8, tile * 8 + 8)
            work_ref[0, at, :] = jnp.where(last, 0.0, whole[at]) - update[at]
        work_ref[0, place, :] = jnp.concatenate(before, axis=0)

    def reduce_panel(base, current):
        inside = jnp.logical_and(lanes >= base, lanes < base + 16)
        picks = [lanes == base + j for j in range(16)]
        cols = [[spread(current[t], pick) for t in range(2)] for pick in picks]
        tiles = [
            jnp.where(inside, (lanes - base == rows + 8 * t).astype(F32), current[t])
            for t in range(2)
        ]
        return inside, picks, tiles, cols

    def keep(solved, gone, at):
        high, low = split2(jnp.concatenate(solved, axis=0))
        high_ref[0, gone, :] = jnp.zeros((16, RANK), BF16)
        low_ref[0, gone, :] = jnp.zeros((16, RANK), BF16)
        high_ref[0, at, :] = high
        low_ref[0, at, :] = low

    def step(panel, carry):
        current, coming, before = carry
        base = panel * 16
        gone = pl.ds(pl.multiple_of(lax.rem(base + ends, RANK), 16), 16)
        following = lax.rem(base + 32, RANK)
        inside, picks, tiles, cols = reduce_panel(base, current)
        earlier = jnp.logical_and(lanes >= base - 16, lanes < base)
        old = [[spread(tile, lanes == base - 16 + j) for j in range(16)] for tile in coming]
        coming = [jnp.where(earlier, 0.0, coming[t]) - combine(old[t], before) for t in range(2)]
        weights = [[spread(tile, pick) for pick in picks] for tile in coming]
        apply_last(base - 16, gone, before)
        solved = panel_solve(tiles, cols, rows)
        keep(solved, gone, pl.ds(pl.multiple_of(base, 16), 16))
        upcoming = tuple(
            jnp.where(inside, 0.0, coming[t]) - combine(weights[t], solved) for t in range(2)
        )
        stale = tuple(
            work_ref[0, pl.ds(pl.multiple_of(following + 8 * t, 8), 8), :] for t in range(2)
        )
        return upcoming, stale, tuple(solved)

    high_ref[0] = jnp.zeros((RANK, RANK), BF16)
    low_ref[0] = jnp.zeros((RANK, RANK), BF16)
    tile_at = lambda start: work_ref[0, start : start + 8, :]
    start = ((tile_at(0), tile_at(8)), (tile_at(16), tile_at(24)), (tile_at(112), tile_at(120)))
    current, _, before = lax.fori_loop(0, RANK // 16 - 1, step, start)
    _, _, tiles, cols = reduce_panel(ends, current)
    apply_last(ends - 16, slice(ends - 16, ends), before)
    solved = panel_solve(tiles, cols, rows)
    keep(solved, slice(ends - 16, ends), slice(ends, RANK))
    apply_last(ends, slice(ends, RANK), solved)


def part(buf_ref, index, slab):
    start = (index % 2) * 4
    return buf_ref[:, start : start + 4, index // 2, slab].reshape(RANK, RANK)


def capacitance(factor, factor_t, grams):
    top = mm_exact_right(grams[0], factor[:RANK])
    low = mm_exact_right(grams[1], factor[RANK:])
    return mm_exact_left(factor_t, jnp.concatenate((top, low), axis=0))


def identity():
    down = lax.broadcasted_iota(jnp.int32, (RANK, RANK), 0)
    return (down == lax.broadcasted_iota(jnp.int32, (RANK, RANK), 1)).astype(F32)


def eliminate(cap, term, work_ref):
    inverse = work_ref[0]
    wide = mm(inverse, cap[:RANK, RANK:])
    cross = cap[RANK:, :RANK]
    work_ref[0] = cap[RANK:, RANK:] + identity() - mm(cross, wide)
    first = mm(inverse, term[:RANK])
    rest = term[RANK:] - mm(cross, first)
    return wide, first, rest


def vmem():
    return pl.BlockSpec(memory_space=pltpu.VMEM)


def shape(*dims, kind=F32):
    return jax.ShapeDtypeStruct(dims, kind)


def inverse_scratch():
    return [
        pltpu.VMEM((1, RANK, RANK), F32),
        pltpu.VMEM((1, RANK, RANK), BF16),
        pltpu.VMEM((1, RANK, RANK), BF16),
    ]


def body(right_side, leaf_inverse, basis_one, basis_two, factor_one, factor_two):
    rows = leaf_inverse.shape[0]
    dma = pltpu.SemaphoreType.DMA
    plane = NZ * NX - 1
    hbm = pl.BlockSpec(memory_space=pltpu.HBM)
    return pl.pallas_call(
        whole_kernel,
        out_shape=shape(64, rows),
        in_specs=[hbm] * 6,
        out_specs=vmem(),
        scratch_shapes=[
            pltpu.VMEM((rows, 2 * RANK), BF16),
            pltpu.VMEM((rows, 2 * RANK), BF16),
            pltpu.VMEM((64, rows), F32),
            pltpu.VMEM((2, RANK, 192), F32),
            pltpu.VMEM((2, 2 * RANK, 192), F32),
            pltpu.VMEM((64, rows), F32),
            pltpu.VMEM((rows, rows), F32),
            pltpu.VMEM((rows, RANK), F32),
            pltpu.VMEM((rows, RANK), F32),
            pltpu.VMEM((NX, NZ, 2, 2, 8, RANK), F32),
            pltpu.VMEM((2, NX, NZ, 8, RANK), F32),
            pltpu.VMEM((NX, NZ, 8, RANK), F32),
            pltpu.VMEM((NZ, NX, 8, RANK), F32),
            pltpu.VMEM((plane, 8, RANK), F32),
            pltpu.VMEM((8, RANK), F32),
            pltpu.VMEM((4, 2, 8, RANK), F32),
        ] + inverse_scratch() + [
            pltpu.VMEM(factor_one.shape, BF16),
            pltpu.VMEM(factor_two.shape, BF16),
            pltpu.VMEM((2 * RANK, 2 * RANK), BF16),
            pltpu.VMEM((2 * RANK, 2 * RANK), BF16),
            pltpu.VMEM((2 * RANK, rows), BF16),
            pltpu.VMEM((2 * RANK, rows), BF16),
            dma((6,)), dma, dma, dma((plane,)), dma((plane,)), dma((8,)), dma((8,)),
            dma((14,)), dma((14,)), dma((9,)), dma((9,)), dma((2,)), dma((2,)),
        ],
        compiler_params=pltpu.CompilerParams(
            collective_id=0, has_side_effects=True, vmem_limit_bytes=56_400_000
        ),
    )(right_side.T, leaf_inverse, basis_one, basis_two, factor_one, factor_two).T


def solution(mesh):
    split = P(("gx", "gy"), None)
    return jax.shard_map(
        body, mesh=mesh, in_specs=(split, split, split, split, P(), P()),
        out_specs=split, check_vma=False,
    )
```
